512 devices in a mesh: row: 32 (over x_lo, y, core), col: 16 (over z, x_hi).
Axes of the slice: x: 4 (x_hi: 2, x_lo: 2; x = x_hi * 2 + x_lo), y: 8, z: 8, core: 2. Of those that a mesh axis runs over, the one named last changes fastest.
Arguments:
- x_slab: float32 [8192, 4096], P('col', 'row'), may hold values from -5400 to 5400, as said below
- weight_c: float32 [1], replicated, may hold values from 2048 to 16384
Outputs:
- trailing: float32 [4096, 4096], P('row', 'col')
- panels: float32 [4096, 512], P('row')
- inverses: float32 [2, 256, 256], replicated
- frobenius: float32 [1], replicated
The draws below stay inside these ranges and needn't reach their ends.
Inputs may be any that keep to these rules, and one draw needn't show every extreme that they name: `x_slab`: real-valued entries.
All inputs are finite; a program needn't handle non-finite values.
Results may differ from the reference program's by a relative error of at most 0.00015.
Values sent between devices are 32-bit elements; how exact they have to be, the bound alone decides.
A program may use at most 64 MiB of HBM per device.

```python
import math
import jax
import jax.numpy as jnp
from jax import lax

W = 4096
PANEL = 256
PANELS = 2
ROWS = 8192


def draw_x_slab(key, part):
    keys = jax.random.split(jax.random.fold_in(key, 17), 3)
    row_scale = 10.0 ** jax.random.uniform(keys[0], (ROWS, 1), jnp.float32) * 3.0 ** (jnp.arange(ROWS, dtype=jnp.float32)[:, None] / ROWS)
    col_scale = 10.0 ** jax.random.uniform(keys[1], (1, W), jnp.float32) * 3.0 ** (jnp.arange(W, dtype=jnp.float32)[None, :] / W)
    base = jnp.clip(jax.random.normal(keys[2], (ROWS, W), jnp.float32), -6.0, 6.0)
    return (base * row_scale * col_scale).astype(jnp.float32)


def setup_inputs(seed: int = 0) -> dict:
    arg_keys = jax.random.split(jax.random.key(seed), 3)
    return {
        "x_slab": draw_x_slab(jax.random.fold_in(arg_keys[2], 71), 0),
        "weight_c": jnp.clip(jnp.exp(jax.random.uniform(arg_keys[1], (1,), jnp.float32, math.log(2048.0), math.log(16384.0))), 2048.0, 16384.0),
    }


HIGH = lax.Precision.HIGHEST

def product(left, right):
    return jnp.dot(left.astype(jnp.float32), right.astype(jnp.float32), preferred_element_type=jnp.float32, precision=HIGH)

def invert_lower(block):
    factor = jnp.linalg.cholesky(block)
    identity = jnp.eye(block.shape[0], dtype=block.dtype)
    return lax.linalg.triangular_solve(factor, identity, left_side=True, lower=True)

def lower_panel(column, inverse, start, row_ids, panel_size):
    values = product(column, inverse.T)
    targets = start + jnp.arange(panel_size, dtype=jnp.int32)
    return jnp.where(row_ids[:, None] >= targets[None, :], values, jnp.zeros_like(values))

def reference(x_slab, weight_c):
    squares = jnp.sum(x_slab * x_slab)
    factor_c = weight_c[0] / squares
    gram = product(x_slab.T, x_slab) * factor_c + jnp.eye(W, dtype=x_slab.dtype)
    row_ids = jnp.arange(W, dtype=jnp.int32)
    matrix = gram
    lowers = []
    inverses = []
    for number in range(PANELS):
        start = number * PANEL
        column = matrix[:, start:start + PANEL]
        inverse = invert_lower(column[start:start + PANEL])
        lower = lower_panel(column, inverse, start, row_ids, PANEL)
        matrix = matrix - product(lower, lower.T)
        lowers.append(lower)
        inverses.append(inverse)
    return (matrix, jnp.concatenate(lowers, axis=1), jnp.stack(inverses), jnp.sqrt(squares).reshape(1))
```

```python
import functools

import jax
import jax.numpy as jnp
from jax import lax
from jax.experimental import pallas as pl
from jax.experimental.pallas import tpu as pltpu
from jax.sharding import Mesh
from jax.sharding import PartitionSpec as P

PANEL = 256
AXES = ("x", "y", "core", "z", "h")
ROW = ("x", "y", "core")
COL = ("z", "h")
HIGH = lax.Precision.HIGHEST
F32 = jnp.float32


def rem(a, n):
    return lax.rem(a + n, n)


def place():
    x, y, k = lax.axis_index("x"), lax.axis_index("y"), lax.axis_index("core")
    z, h = lax.axis_index("z"), lax.axis_index("h")
    return x, y, k, z, h


def gram_kernel(
    x_ref, tile_ref, ga_ref, gb_ref, d_ref, sq_ref,
    xb, other, lhs, prod, stage, landed, mine, ring, parts, flip, pile, turned, half, sq2,
    s_ring, r_ring, s_core, r_core, s_rs, r_rs, s_pl, r_pl, s_ag, r_ag, s_a2a, r_a2a, s_t, r_t,
):
    x, y, k, z, h = place()
    a = x * 8 + y
    b = z * 2 + h
    gap = rem(b - a, 16)

    def at_a(i):
        return (lax.div(i, 8), lax.rem(i, 8), k, z, h)

    def at_b(i):
        return (x, y, k, lax.div(i, 2), lax.rem(i, 2))

    partner = (x, y, 1 - k, z, h)
    mirror = (lax.div(b, 8), lax.rem(b, 8), k, lax.div(a, 2), lax.rem(a, 2))

    def copy(src, dst, ssem, rsem, dev):
        return pltpu.make_async_remote_copy(
            src_ref=src, dst_ref=dst, send_sem=ssem, recv_sem=rsem,
            device_id=dev, device_id_type=pl.DeviceIdType.MESH,
        )

    barrier = pltpu.get_barrier_semaphore()

    def signal(dev):
        pl.semaphore_signal(barrier, inc=1, device_id=dev, device_id_type=pl.DeviceIdType.MESH)

    @pl.loop(1, 16)
    def _(i):
        signal(at_a(lax.rem(a + i, 16)))
        signal(at_b(lax.rem(b + i, 16)))

    signal(partner)

    @pl.when(a != b)
    def _():
        signal(mirror)

    @pl.when(a != b)
    def _():
        pl.semaphore_wait(barrier, 32)

    @pl.when(a == b)
    def _():
        pl.semaphore_wait(barrier, 31)

    sgn = 1 - 2 * k

    def slot(xx, dy):
        return xx * 8 + rem(y + dy + 8, 8)

    def pass_on(src, who, to, n):
        return copy(src, xb.at[who], s_ring.at[n], r_ring.at[who], to)

    def y_at(dy):
        return (x, rem(y + dy + 8, 8), k, z, h)

    across = (1 - x, y, k, z, h)
    sent = []

    def go(who, to, src=None):
        c = pass_on(xb.at[who] if src is None else src, who, to, len(sent))
        c.start()
        sent.append(c)

    def arrive(who):
        pass_on(xb.at[who], who, across, 0).wait_recv()

    go(a, y_at(1), x_ref)
    go(a, y_at(-1), x_ref)
    go(a, across, x_ref)
    to_core = copy(x_ref, other, s_core.at[0], r_core.at[0], partner)
    to_core.start()
    xb[a] = x_ref[...]
    arrive(slot(x, -1))
    go(slot(x, -1), y_at(1))
    go(slot(x, -1), across)
    arrive(slot(x, 1))
    go(slot(x, 1), y_at(-1))
    go(slot(x, 1), across)
    to_core.wait_recv()
    lhs[:, pl.ds(pl.multiple_of(k * 128, 128), 128)] = x_ref[...]
    lhs[:, pl.ds(pl.multiple_of((1 - k) * 128, 128), 128)] = other[...]
    arrive(slot(1 - x, 0))
    arrive(slot(x, -2))
    go(slot(x, -2), y_at(1))
    arrive(slot(x, 2))
    go(slot(x, 2), y_at(-1))
    arrive(slot(1 - x, -1))
    go(slot(1 - x, -1), y_at(1))
    arrive(slot(1 - x, 1))
    go(slot(1 - x, 1), y_at(-1))
    arrive(slot(x, -3))
    arrive(slot(x, 3))
    go(slot(x, -3 * sgn), y_at(sgn))
    arrive(slot(1 - x, -2))
    go(slot(1 - x, -2), y_at(1))
    arrive(slot(1 - x, 2))
    go(slot(1 - x, 2), y_at(-1))
    arrive(slot(1 - x, -3))
    arrive(slot(1 - x, 3))
    go(slot(1 - x, -3 * sgn), y_at(sgn))
    arrive(slot(x, 4))
    arrive(slot(1 - x, 4))

    def multiply(i, total):
        blk = xb[i]
        prod[i] = lax.dot_general(
            blk, lhs[...], (((0,), (0,)), ((), ())), precision=HIGH, preferred_element_type=F32
        )
        return total + jnp.sum((blk * blk).reshape(64, 8, 128), axis=0)

    total = lax.fori_loop(0, 16, multiply, jnp.zeros((8, 128), F32))
    for i in range(16):
        stage[i, 0:16, :] = prod[i // 8, (i % 8) * 16 : (i % 8) * 16 + 16, :]
        stage[i, 16:24, 0:128] = total
        stage[i, 16:24, 128:256] = jnp.zeros((8, 128), F32)

    def rs(i):
        to = lax.rem(b + i, 16)
        return copy(stage.at[to], landed.at[b], s_rs.at[i], r_rs.at[b], at_b(to))

    def rs_from(i):
        who = lax.rem(b + i, 16)
        return copy(stage.at[who], landed.at[who], s_rs.at[i], r_rs.at[who], at_b(who))

    @pl.loop(1, 16)
    def _(i):
        rs(i).start()

    landed[b] = stage[b]

    @pl.loop(1, 16)
    def _(i):
        rs_from(i).wait_recv()

    red = landed[0]
    for i in range(1, 16):
        red = red + landed[i]
    mine[0:16, :] = red[0:16]
    sq_ref[...] = red[16:24]

    def spread(i):
        to = lax.rem(a + i, 16)
        rows = pl.ds(pl.multiple_of(16 + 16 * a, 16), 16)
        return copy(mine.at[0:16], mine.at[rows], s_pl.at[i], r_pl.at[a], at_a(to))

    @pl.when(a < 2)
    def _():
        @pl.loop(1, 16)
        def _(i):
            spread(i).start()

        mine[pl.ds(pl.multiple_of(16 + 16 * a, 16), 16), :] = red[0:16]

    for i in range(2):

        @pl.when(a != i)
        def _():
            copy(mine.at[0:16], mine.at[16 + 16 * i : 32 + 16 * i], s_pl.at[0], r_pl.at[i], across).wait_recv()

    def ag(i):
        to = lax.rem(b + i, 16)
        return copy(mine, ring.at[b], s_ag.at[i], r_ag.at[b], at_b(to))

    def ag_from(i):
        who = lax.rem(b + i, 16)
        return copy(mine, ring.at[who], s_ag.at[i], r_ag.at[who], at_b(who))

    @pl.loop(1, 16)
    def _(i):
        ag(i).start()

    ring[b] = mine[...]

    def tile(d):
        to = lax.rem(a + d, 16)
        return to, copy(prod.at[to], pile.at[b], s_a2a.at[d], r_a2a.at[b], at_b(to))

    @pl.loop(0, 9)
    def _(d):
        to, c = tile(d)

        @pl.when(to != b)
        def _():
            c.start()

    @pl.loop(1, 16)
    def _(i):
        ag_from(i).wait_recv()

    for i in range(16):
        r = (i % 8) * 16
        for j in range(3):
            parts[k, j, i // 8, r : r + 16, :] = ring[i, 16 * j : 16 * j + 16, :]
    swap = copy(parts.at[k], parts.at[k], s_core.at[1], r_core.at[1], partner)
    swap_in = copy(parts.at[1 - k], parts.at[1 - k], s_core.at[1], r_core.at[1], partner)
    swap.start()
    swap_sq = copy(sq_ref, sq2, s_core.at[2], r_core.at[2], partner)
    swap_sq.start()
    send_flip = copy(parts.at[k, 0], flip.at[k], s_t.at[0], r_t.at[0], mirror)

    @pl.when(a != b)
    def _():
        send_flip.start()

    @pl.when(a == b)
    def _():
        flip[k] = parts[k, 0]

    swap_in.wait_recv()
    swap_sq.wait()
    sq_ref[...] = sq_ref[...] + sq2[...]
    for kk in range(2):
        for i in range(2):
            r = i * 256 + kk * 128
            ga_ref[r : r + 128, :] = parts[kk, 0, i]
            for j in range(2):
                d_ref[r : r + 128, 256 * j : 256 * j + 256] = parts[kk, 1 + j, i]

    @pl.when(a != b)
    def _():
        send_flip.wait_recv()

    flop = copy(flip.at[k], flip.at[k], s_core.at[3], r_core.at[3], partner)
    flop_in = copy(flip.at[1 - k], flip.at[1 - k], s_core.at[3], r_core.at[3], partner)
    flop.start()

    send_turn = copy(turned, half, s_t.at[1], r_t.at[1], mirror)
    trade = copy(
        turned.at[:, pl.ds(pl.multiple_of((1 - k) * 128, 128), 128)],
        half.at[:, 0:128],
        s_core.at[4], r_core.at[4], partner,
    )

    @pl.when(gap <= 8)
    def _():
        pile[b] = prod[b]

        @pl.loop(1, 16)
        def _(i):
            who = lax.rem(b + i, 16)
            copy(prod.at[who], pile.at[who], s_a2a.at[0], r_a2a.at[who], at_b(who)).wait_recv()

        total_tile = pile[0]
        for i in range(1, 16):
            total_tile = total_tile + pile[i]
        turned[...] = total_tile
        trade.start()

        @pl.when((gap >= 1) & (gap <= 7))
        def _():
            send_turn.start()

        own = turned[:, pl.ds(pl.multiple_of(k * 128, 128), 128)]
        tile_ref[:, pl.ds(pl.multiple_of(k * 128, 128), 128)] = own.T
        trade.wait_recv()
        tile_ref[:, pl.ds(pl.multiple_of((1 - k) * 128, 128), 128)] = half[:, 0:128].T
        trade.wait_send()

        @pl.when((gap >= 1) & (gap <= 7))
        def _():
            send_turn.wait_send()

    @pl.when(gap >= 9)
    def _():
        send_turn.wait_recv()
        tile_ref[...] = half[...]

    flop_in.wait_recv()
    for kk in range(2):
        for i in range(2):
            r = i * 256 + kk * 128
            gb_ref[r : r + 128, :] = flip[kk, i]

    for c in sent:
        c.wait_send()
    to_core.wait_send()
    swap.wait_send()
    flop.wait_send()

    @pl.when(a != b)
    def _():
        send_flip.wait_send()

    @pl.when(a < 2)
    def _():
        @pl.loop(1, 16)
        def _(i):
            spread(i).wait_send()

    @pl.loop(1, 16)
    def _(i):
        rs(i).wait_send()
        ag(i).wait_send()

    @pl.loop(0, 9)
    def _(d):
        to, c = tile(d)

        @pl.when(to != b)
        def _():
            c.wait_send()


def gram_parts(x_slab):
    vmem = pl.BlockSpec(memory_space=pltpu.VMEM)
    dma = pltpu.SemaphoreType.DMA
    shapes = [(128, 256), (512, 256), (512, 256), (512, 512), (8, 256)]
    return pl.pallas_call(
        gram_kernel,
        out_shape=[jax.ShapeDtypeStruct(s, F32) for s in shapes],
        in_specs=[vmem],
        out_specs=[vmem] * 5,
        scratch_shapes=[
            pltpu.VMEM((16, 512, 128), F32),
            pltpu.VMEM((512, 128), F32),
            pltpu.VMEM((512, 256), F32),
            pltpu.VMEM((16, 128, 256), F32),
            pltpu.VMEM((16, 24, 256), F32),
            pltpu.VMEM((16, 24, 256), F32),
            pltpu.VMEM((48, 256), F32),
            pltpu.VMEM((16, 48, 256), F32),
            pltpu.VMEM((2, 3, 2, 128, 256), F32),
            pltpu.VMEM((2, 2, 128, 256), F32),
            pltpu.VMEM((16, 128, 256), F32),
            pltpu.VMEM((128, 256), F32),
            pltpu.VMEM((128, 256), F32),
            pltpu.VMEM((8, 256), F32),
            dma((20,)), dma((16,)),
            dma((5,)), dma((5,)),
            dma((16,)), dma((16,)),
            dma((16,)), dma((2,)),
            dma((16,)), dma((16,)),
            dma((9,)), dma((16,)),
            dma((2,)), dma((2,)),
        ],
        compiler_params=pltpu.CompilerParams(
            collective_id=0, has_side_effects=True, vmem_limit_bytes=40 * 1024 * 1024
        ),
        name="gram_parts",
    )(x_slab)


def product(left, right):
    return jnp.dot(left, right, preferred_element_type=F32, precision=HIGH)


def invert_lower(block):
    factor = jnp.linalg.cholesky(block)
    identity = jnp.eye(block.shape[0], dtype=block.dtype)
    return lax.linalg.triangular_solve(factor, identity, left_side=True, lower=True)


def on_device(x_slab, weight_c):
    x, y, k, z, h = place()
    a = x * 8 + y
    b = z * 2 + h
    tile, ga, gb, diag, sq = gram_parts(x_slab)
    squares = jnp.sum(sq)
    factor_c = weight_c[0] / squares
    rows = a * 256 + k * 128 + jnp.arange(128, dtype=jnp.int32)
    cols = b * 256 + jnp.arange(256, dtype=jnp.int32)
    ids = jnp.concatenate([rows, cols])
    first = jnp.arange(512, dtype=jnp.int32)
    both = jnp.concatenate([lax.dynamic_slice_in_dim(ga, k * 128, 128, 1), gb], axis=1)
    both = both * factor_c + (first[:, None] == ids[None, :]).astype(F32)
    diag = diag * factor_c + jnp.eye(512, dtype=F32)
    gram = tile * factor_c + (rows[:, None] == cols[None, :]).astype(F32)
    inv1 = invert_lower(diag[:256, :256])
    cross = product(diag[256:, :256], inv1.T)
    inv2 = invert_lower(diag[256:, 256:] - product(cross, cross.T))
    low1 = product(inv1, both[:256])
    low1 = jnp.where(ids[None, :] >= first[:256, None], low1, 0.0)
    low2 = product(inv2, both[256:] - product(cross, low1))
    low2 = jnp.where(ids[None, :] >= first[256:, None], low2, 0.0)
    low = jnp.concatenate([low1, low2], axis=0)
    out = gram - lax.dot_general(
        low[:, :128], low[:, 128:], (((0,), (0,)), ((), ())), precision=HIGH, preferred_element_type=F32
    )
    return out, low[:, :128].T, jnp.stack([inv1, inv2]), jnp.sqrt(squares).reshape(1)


def solution(mesh):
    split = Mesh(mesh.devices.reshape(2, 8, 2, 8, 2), AXES)
    return jax.shard_map(
        on_device, mesh=split, in_specs=(P(COL, ROW), P()),
        out_specs=(P(ROW, COL), P(ROW, None), P(), P()), check_vma=False,
    )
```

```python
import functools

import jax
import jax.numpy as jnp
from jax import lax
from jax.experimental import pallas as pl
from jax.experimental.pallas import tpu as pltpu
from jax.sharding import Mesh
from jax.sharding import PartitionSpec as P

PANEL = 256
AXES = ("x", "y", "core", "z", "h")
ROW = ("x", "y", "core")
COL = ("z", "h")
HIGH = lax.Precision.HIGHEST
F32 = jnp.float32


def rem(a, n):
    return lax.rem(a + n, n)


def place():
    x, y, k = lax.axis_index("x"), lax.axis_index("y"), lax.axis_index("core")
    z, h = lax.axis_index("z"), lax.axis_index("h")
    return x, y, k, z, h


def gram_kernel(
    x_ref, tile_ref, ga_ref, gb_ref, d_ref, sq_ref,
    xb, other, lhs, prod, stage, landed, mine, ring, parts, flip, pile, turned, half, sq2,
    s_ring, r_ring, s_core, r_core, s_rs, r_rs, s_pl, r_pl, s_ag, r_ag, s_a2a, r_a2a, s_t, r_t,
):
    x, y, k, z, h = place()
    a = x * 8 + y
    b = z * 2 + h
    gap = rem(b - a, 16)

    def at_a(i):
        return (lax.div(i, 8), lax.rem(i, 8), k, z, h)

    def at_b(i):
        return (x, y, k, lax.div(i, 2), lax.rem(i, 2))

    partner = (x, y, 1 - k, z, h)
    mirror = (lax.div(b, 8), lax.rem(b, 8), k, lax.div(a, 2), lax.rem(a, 2))

    def copy(src, dst, ssem, rsem, dev):
        return pltpu.make_async_remote_copy(
            src_ref=src, dst_ref=dst, send_sem=ssem, recv_sem=rsem,
            device_id=dev, device_id_type=pl.DeviceIdType.MESH,
        )

    barrier = pltpu.get_barrier_semaphore()

    def signal(dev):
        pl.semaphore_signal(barrier, inc=1, device_id=dev, device_id_type=pl.DeviceIdType.MESH)

    @pl.loop(1, 16)
    def _(i):
        signal(at_a(lax.rem(a + i, 16)))
        signal(at_b(lax.rem(b + i, 16)))

    signal(partner)

    @pl.when(a != b)
    def _():
        signal(mirror)

    @pl.when(a != b)
    def _():
        pl.semaphore_wait(barrier, 32)

    @pl.when(a == b)
    def _():
        pl.semaphore_wait(barrier, 31)

    sgn = 1 - 2 * k

    def slot(xx, dy):
        return xx * 8 + rem(y + dy + 8, 8)

    def pass_on(src, who, to, n):
        return copy(src, xb.at[who], s_ring.at[n], r_ring.at[who], to)

    def y_at(dy):
        return (x, rem(y + dy + 8, 8), k, z, h)

    across = (1 - x, y, k, z, h)
    sent = []

    def go(who, to, src=None):
        c = pass_on(xb.at[who] if src is None else src, who, to, len(sent))
        c.start()
        sent.append(c)

    def arrive(who):
        pass_on(xb.at[who], who, across, 0).wait_recv()

    go(a, y_at(1), x_ref)
    go(a, y_at(-1), x_ref)
    go(a, across, x_ref)
    to_core = copy(x_ref, other, s_core.at[0], r_core.at[0], partner)
    to_core.start()
    xb[a] = x_ref[...]
    arrive(slot(x, -1))
    go(slot(x, -1), y_at(1))
    go(slot(x, -1), across)
    arrive(slot(x, 1))
    go(slot(x, 1), y_at(-1))
    go(slot(x, 1), across)
    to_core.wait_recv()
    lhs[:, pl.ds(pl.multiple_of(k * 128, 128), 128)] = x_ref[...]
    lhs[:, pl.ds(pl.multiple_of((1 - k) * 128, 128), 128)] = other[...]
    arrive(slot(1 - x, 0))
    arrive(slot(x, -2))
    go(slot(x, -2), y_at(1))
    arrive(slot(x, 2))
    go(slot(x, 2), y_at(-1))
    arrive(slot(1 - x, -1))
    go(slot(1 - x, -1), y_at(1))
    arrive(slot(1 - x, 1))
    go(slot(1 - x, 1), y_at(-1))
    arrive(slot(x, -3))
    arrive(slot(x, 3))
    go(slot(x, -3 * sgn), y_at(sgn))
    arrive(slot(1 - x, -2))
    go(slot(1 - x, -2), y_at(1))
    arrive(slot(1 - x, 2))
    go(slot(1 - x, 2), y_at(-1))
    arrive(slot(1 - x, -3))
    arrive(slot(1 - x, 3))
    go(slot(1 - x, -3 * sgn), y_at(sgn))
    arrive(slot(x, 4))
    arrive(slot(1 - x, 4))

    def multiply(i, total):
        blk = xb[i]
        prod[i] = lax.dot_general(
            blk, lhs[...], (((0,), (0,)), ((), ())), precision=HIGH, preferred_element_type=F32
        )
        return total + jnp.sum((blk * blk).reshape(64, 8, 128), axis=0)

    total = lax.fori_loop(0, 16, multiply, jnp.zeros((8, 128), F32))
    for i in range(16):
        stage[i, 0:16, :] = prod[i // 8, (i % 8) * 16 : (i % 8) * 16 + 16, :]
        stage[i, 16:24, 0:128] = total
        stage[i, 16:24, 128:256] = jnp.zeros((8, 128), F32)

    def rs(i):
        to = lax.rem(b + i, 16)
        return copy(stage.at[to], landed.at[b], s_rs.at[i], r_rs.at[b], at_b(to))

    def rs_from(i):
        who = lax.rem(b + i, 16)
        return copy(stage.at[who], landed.at[who], s_rs.at[i], r_rs.at[who], at_b(who))

    @pl.loop(1, 16)
    def _(i):
        rs(i).start()

    landed[b] = stage[b]

    @pl.loop(1, 16)
    def _(i):
        rs_from(i).wait_recv()

    red = landed[0]
    for i in range(1, 16):
        red = red + landed[i]
    mine[0:16, :] = red[0:16]
    sq_ref[...] = red[16:24]

    def spread(i):
        to = lax.rem(a + i, 16)
        rows = pl.ds(pl.multiple_of(16 + 16 * a, 16), 16)
        return copy(mine.at[0:16], mine.at[rows], s_pl.at[i], r_pl.at[a], at_a(to))

    @pl.when(a < 2)
    def _():
        @pl.loop(1, 16)
        def _(i):
            spread(i).start()

        mine[pl.ds(pl.multiple_of(16 + 16 * a, 16), 16), :] = red[0:16]

    for i in range(2):

        @pl.when(a != i)
        def _():
            copy(mine.at[0:16], mine.at[16 + 16 * i : 32 + 16 * i], s_pl.at[0], r_pl.at[i], across).wait_recv()

    def ag(i):
        to = lax.rem(b + i, 16)
        return copy(mine, ring.at[b], s_ag.at[i], r_ag.at[b], at_b(to))

    def ag_from(i):
        who = lax.rem(b + i, 16)
        return copy(mine, ring.at[who], s_ag.at[i], r_ag.at[who], at_b(who))

    @pl.loop(1, 16)
    def _(i):
        ag(i).start()

    ring[b] = mine[...]

    def tile(d):
        to = lax.rem(a + d, 16)
        return to, copy(prod.at[to], pile.at[b], s_a2a.at[d], r_a2a.at[b], at_b(to))

    @pl.loop(0, 9)
    def _(d):
        to, c = tile(d)

        @pl.when(to != b)
        def _():
            c.start()

    @pl.loop(1, 16)
    def _(i):
        ag_from(i).wait_recv()

    for i in range(16):
        r = (i % 8) * 16
        for j in range(3):
            parts[k, j, i // 8, r : r + 16, :] = ring[i, 16 * j : 16 * j + 16, :]
    swap = copy(parts.at[k], parts.at[k], s_core.at[1], r_core.at[1], partner)
    swap_in = copy(parts.at[1 - k], parts.at[1 - k], s_core.at[1], r_core.at[1], partner)
    swap.start()
    swap_sq = copy(sq_ref, sq2, s_core.at[2], r_core.at[2], partner)
    swap_sq.start()
    send_flip = copy(parts.at[k, 0], flip.at[k], s_t.at[0], r_t.at[0], mirror)

    @pl.when(a != b)
    def _():
        send_flip.start()

    @pl.when(a == b)
    def _():
        flip[k] = parts[k, 0]

    swap_in.wait_recv()
    swap_sq.wait()
    sq_ref[...] = sq_ref[...] + sq2[...]
    for kk in range(2):
        for i in range(2):
            r = i * 256 + kk * 128
            ga_ref[r : r + 128, :] = parts[kk, 0, i]
            for j in range(2):
                d_ref[r : r + 128, 256 * j : 256 * j + 256] = parts[kk, 1 + j, i]

    @pl.when(a != b)
    def _():
        send_flip.wait_recv()

    flop = copy(flip.at[k], flip.at[k], s_core.at[3], r_core.at[3], partner)
    flop_in = copy(flip.at[1 - k], flip.at[1 - k], s_core.at[3], r_core.at[3], partner)
    flop.start()

    send_turn = copy(turned, half, s_t.at[1], r_t.at[1], mirror)
    trade = copy(
        turned.at[:, pl.ds(pl.multiple_of((1 - k) * 128, 128), 128)],
        half.at[:, 0:128],
        s_core.at[4], r_core.at[4], partner,
    )

    @pl.when(gap <= 8)
    def _():
        pile[b] = prod[b]

        @pl.loop(1, 16)
        def _(i):
            who = lax.rem(b + i, 16)
            copy(prod.at[who], pile.at[who], s_a2a.at[0], r_a2a.at[who], at_b(who)).wait_recv()

        total_tile = pile[0]
        for i in range(1, 16):
            total_tile = total_tile + pile[i]
        turned[...] = total_tile
        trade.start()

        @pl.when((gap >= 1) & (gap <= 7))
        def _():
            send_turn.start()

        own = turned[:, pl.ds(pl.multiple_of(k * 128, 128), 128)]
        tile_ref[:, pl.ds(pl.multiple_of(k * 128, 128), 128)] = own.T
        trade.wait_recv()
        tile_ref[:, pl.ds(pl.multiple_of((1 - k) * 128, 128), 128)] = half[:, 0:128].T
        trade.wait_send()

        @pl.when((gap >= 1) & (gap <= 7))
        def _():
            send_turn.wait_send()

    @pl.when(gap >= 9)
    def _():
        send_turn.wait_recv()
        tile_ref[...] = half[...]

    flop_in.wait_recv()
    for kk in range(2):
        for i in range(2):
            r = i * 256 + kk * 128
            gb_ref[r : r + 128, :] = flip[kk, i]

    for c in sent:
        c.wait_send()
    to_core.wait_send()
    swap.wait_send()
    flop.wait_send()

    @pl.when(a != b)
    def _():
        send_flip.wait_send()

    @pl.when(a < 2)
    def _():
        @pl.loop(1, 16)
        def _(i):
            spread(i).wait_send()

    @pl.loop(1, 16)
    def _(i):
        rs(i).wait_send()
        ag(i).wait_send()

    @pl.loop(0, 9)
    def _(d):
        to, c = tile(d)

        @pl.when(to != b)
        def _():
            c.wait_send()


def gram_parts(x_slab):
    vmem = pl.BlockSpec(memory_space=pltpu.VMEM)
    dma = pltpu.SemaphoreType.DMA
    shapes = [(128, 256), (512, 256), (512, 256), (512, 512), (8, 256)]
    return pl.pallas_call(
        gram_kernel,
        out_shape=[jax.ShapeDtypeStruct(s, F32) for s in shapes],
        in_specs=[vmem],
        out_specs=[vmem] * 5,
        scratch_shapes=[
            pltpu.VMEM((16, 512, 128), F32),
            pltpu.VMEM((512, 128), F32),
            pltpu.VMEM((512, 256), F32),
            pltpu.VMEM((16, 128, 256), F32),
            pltpu.VMEM((16, 24, 256), F32),
            pltpu.VMEM((16, 24, 256), F32),
            pltpu.VMEM((48, 256), F32),
            pltpu.VMEM((16, 48, 256), F32),
            pltpu.VMEM((2, 3, 2, 128, 256), F32),
            pltpu.VMEM((2, 2, 128, 256), F32),
            pltpu.VMEM((16, 128, 256), F32),
            pltpu.VMEM((128, 256), F32),
            pltpu.VMEM((128, 256), F32),
            pltpu.VMEM((8, 256), F32),
            dma((20,)), dma((16,)),
            dma((5,)), dma((5,)),
            dma((16,)), dma((16,)),
            dma((16,)), dma((2,)),
            dma((16,)), dma((16,)),
            dma((9,)), dma((16,)),
            dma((2,)), dma((2,)),
        ],
        compiler_params=pltpu.CompilerParams(
            collective_id=0, has_side_effects=True, vmem_limit_bytes=40 * 1024 * 1024
        ),
        name="gram_parts",
    )(x_slab)


def eliminate(get, put, n=128, nb=8):
    lane = lax.broadcasted_iota(jnp.int32, (8, n), 1)
    sub = lax.broadcasted_iota(jnp.int32, (8, n), 0)
    tiles = [get(t) for t in range(n // 8)]
    for j0 in range(0, n, nb):
        t0 = j0 // 8
        tn = nb // 8
        live = range(t0, n // 8)
        cols = {}
        for l in range(nb):
            for t in live:
                cols[l, t] = jnp.broadcast_to(tiles[t][:, j0 + l : j0 + l + 1], (8, n))
        mult = {}
        inv = []
        for l in range(nb):
            tl, rl = t0 + l // 8, l % 8
            piv = jnp.broadcast_to(cols[l, tl][rl : rl + 1, :], (8, n))
            r = 1.0 / piv
            inv.append(piv)
            for t in live:
                if t < tl:
                    continue
                m = cols[l, t] * r
                if t == tl:
                    m = jnp.where(sub > rl, m, 0.0)
                mult[l, t] = m
            for q in range(l + 1, nb):
                tq, rq = t0 + q // 8, q % 8
                s = jnp.broadcast_to(cols[l, tq][rq : rq + 1, :], (8, n))
                for t in live:
                    if t < tq:
                        continue
                    cols[q, t] = cols[q, t] - mult[l, t] * s
        rows = []
        for l in range(nb):
            tl, rl = t0 + l // 8, l % 8
            piv_row = jnp.where(lane == j0 + l, 1.0, jnp.broadcast_to(tiles[tl][rl : rl + 1, :], (8, n)))
            rows.append(piv_row)
            for t in range(tl, t0 + tn):
                keep = tiles[t]
                if t == tl:
                    zeroed = jnp.where((lane == j0 + l) & (sub > rl), 0.0, keep)
                    tiles[t] = zeroed - mult[l, t] * piv_row
                else:
                    tiles[t] = jnp.where(lane == j0 + l, 0.0, keep) - mult[l, t] * piv_row
            tiles[tl] = jnp.where((sub == rl), piv_row, tiles[tl])
        inside = (lane >= j0) & (lane < j0 + nb)
        masked = [jnp.where((lane > j0 + l) & (lane < j0 + nb), 0.0, rows[l]) for l in range(nb)]
        for t in range(t0 + tn, n // 8):
            acc = jnp.where(inside, 0.0, tiles[t])
            for l in range(nb):
                acc = acc - mult[l, t] * masked[l]
            tiles[t] = acc
        for l in range(nb):
            tl, rl = t0 + l // 8, l % 8
            tiles[tl] = jnp.where(sub == rl, tiles[tl] * lax.rsqrt(inv[l]), tiles[tl])
        for t in range(t0, t0 + tn):
            rr = sub + 8 * t
            put(t, jnp.where(lane <= rr, tiles[t], 0.0))


def dot(left, right, ca=1, cb=0):
    return lax.dot_general(
        left, right, (((ca,), (cb,)), ((), ())), precision=HIGH, preferred_element_type=F32
    )


def factor_pair(s, inv_ref, cross_ref, w):
    def half():
        def put(t, v):
            w[8 * t : 8 * t + 8, :] = v

        eliminate(lambda t: w[8 * t : 8 * t + 8, :], put)

    @pl.loop(0, 2)
    def _(p):
        base = pl.multiple_of(p * 256, 256)
        top, low = pl.ds(base, 128), pl.ds(base + 128, 128)
        w[...] = s[top, top]
        half()
        i11 = w[...]
        l21 = dot(s[low, top], i11, 1, 1)
        w[...] = s[low, low] - dot(l21, l21, 1, 1)
        half()
        i22 = w[...]
        inv_ref[p, 0:128, 0:128] = i11
        inv_ref[p, 0:128, 128:256] = jnp.zeros((128, 128), F32)
        inv_ref[p, 128:256, 128:256] = i22
        inv_ref[p, 128:256, 0:128] = -dot(i22, dot(l21, i11))

        @pl.when(p == 0)
        def _():
            c = dot(s[256:512, 0:256], inv_ref[0], 1, 1)
            cross_ref[...] = c
            s[256:512, 256:512] = s[256:512, 256:512] - dot(c, c, 1, 1)


def finish_kernel(
    weight_ref, tile_ref, ga_ref, gb_ref, d_ref, sq_ref, out_ref, pan_ref, inv_ref, fro_ref,
    s, w, cross, g, low,
):
    x, y, k, z, h = place()
    row0 = (x * 8 + y) * 256 + k * 128
    col0 = (z * 2 + h) * 256
    squares = jnp.sum(jnp.sum(sq_ref[...], axis=0, keepdims=True), axis=1, keepdims=True)
    fro_ref[0] = jnp.sqrt(squares)[0, 0]
    scale = weight_ref[0] / squares

    def iota(shape, dim, start=0):
        return lax.broadcasted_iota(jnp.int32, shape, dim) + start

    def scaled(v, r0, c0):
        eye = (iota(v.shape, 0, r0) == iota(v.shape, 1, c0)).astype(F32)
        return v * scale + eye

    s[...] = scaled(d_ref[...], 0, 0)
    g[:, 0:128] = scaled(ga_ref[:, pl.ds(pl.multiple_of(k * 128, 128), 128)], 0, row0)
    g[:, 128:384] = scaled(gb_ref[...], 0, col0)
    factor_pair(s, inv_ref, cross, w)
    lane = iota((256, 384), 1)
    ids = lane + jnp.where(lane < 128, row0, col0 - 128)
    first = iota((256, 384), 0)
    one = jnp.where(ids >= first, dot(inv_ref[0], g[0:256, :]), 0.0)
    low[0:256, :] = one
    two = dot(inv_ref[1], g[256:512, :] - dot(cross[...], one))
    low[256:512, :] = jnp.where(ids >= first + 256, two, 0.0)
    out_ref[...] = scaled(tile_ref[...], row0, col0) - dot(low[:, 0:128], low[:, 128:384], 0, 0)
    pan_ref[...] = low[:, 0:128].T


def finish(weight_c, tile, ga, gb, diag, sq):
    vmem, smem = pl.BlockSpec(memory_space=pltpu.VMEM), pl.BlockSpec(memory_space=pltpu.SMEM)
    shapes = [(128, 256), (128, 512), (2, 256, 256), (1,)]
    return pl.pallas_call(
        finish_kernel,
        out_shape=[jax.ShapeDtypeStruct(s, F32) for s in shapes],
        in_specs=[smem] + [vmem] * 5,
        out_specs=[vmem] * 3 + [smem],
        scratch_shapes=[
            pltpu.VMEM((512, 512), F32),
            pltpu.VMEM((128, 128), F32),
            pltpu.VMEM((256, 256), F32),
            pltpu.VMEM((512, 384), F32),
            pltpu.VMEM((512, 384), F32),
        ],
        compiler_params=pltpu.CompilerParams(vmem_limit_bytes=40 * 1024 * 1024),
        name="finish",
    )(weight_c, tile, ga, gb, diag, sq)


def on_device(x_slab, weight_c):
    return finish(weight_c, *gram_parts(x_slab))


def solution(mesh):
    split = Mesh(mesh.devices.reshape(2, 8, 2, 8, 2), AXES)
    return jax.shard_map(
        on_device, mesh=split, in_specs=(P(COL, ROW), P()),
        out_specs=(P(ROW, COL), P(ROW, None), P(), P()), check_vma=False,
    )
```

```python
import jax
import jax.numpy as jnp
from jax import lax
from jax.experimental import pallas as pl
from jax.experimental.pallas import tpu as pltpu
from jax.sharding import Mesh
from jax.sharding import PartitionSpec as P

AXES = ("x", "y", "core", "z", "h")
ROW = ("x", "y", "core")
COL = ("z", "h")
HIGH = lax.Precision.HIGHEST
F32 = jnp.float32


def place():
    x, y, k = lax.axis_index("x"), lax.axis_index("y"), lax.axis_index("core")
    z, h = lax.axis_index("z"), lax.axis_index("h")
    return x, y, k, z, h


def dot(left, right, ca=1, cb=0):
    return lax.dot_general(
        left, right, (((ca,), (cb,)), ((), ())), precision=HIGH, preferred_element_type=F32
    )


def eliminate(get, put, n=128, nb=8):
    lane = lax.broadcasted_iota(jnp.int32, (8, n), 1)
    sub = lax.broadcasted_iota(jnp.int32, (8, n), 0)
    tiles = [get(t) for t in range(n // 8)]
    for j0 in range(0, n, nb):
        t0 = j0 // 8
        tn = nb // 8
        live = range(t0, n // 8)
        cols = {}
        for l in range(nb):
            for t in live:
                cols[l, t] = jnp.broadcast_to(tiles[t][:, j0 + l : j0 + l + 1], (8, n))
        mult = {}
        inv = []
        for l in range(nb):
            tl, rl = t0 + l // 8, l % 8
            piv = jnp.broadcast_to(cols[l, tl][rl : rl + 1, :], (8, n))
            r = 1.0 / piv
            inv.append(piv)
            for t in live:
                if t < tl:
                    continue
                m = cols[l, t] * r
                if t == tl:
                    m = jnp.where(sub > rl, m, 0.0)
                mult[l, t] = m
            for q in range(l + 1, nb):
                tq, rq = t0 + q // 8, q % 8
                s = jnp.broadcast_to(cols[l, tq][rq : rq + 1, :], (8, n))
                for t in live:
                    if t < tq:
                        continue
                    cols[q, t] = cols[q, t] - mult[l, t] * s
        rows = []
        for l in range(nb):
            tl, rl = t0 + l // 8, l % 8
            piv_row = jnp.where(lane == j0 + l, 1.0, jnp.broadcast_to(tiles[tl][rl : rl + 1, :], (8, n)))
            rows.append(piv_row)
            for t in range(tl, t0 + tn):
                keep = tiles[t]
                if t == tl:
                    zeroed = jnp.where((lane == j0 + l) & (sub > rl), 0.0, keep)
                    tiles[t] = zeroed - mult[l, t] * piv_row
                else:
                    tiles[t] = jnp.where(lane == j0 + l, 0.0, keep) - mult[l, t] * piv_row
            tiles[tl] = jnp.where((sub == rl), piv_row, tiles[tl])
        inside = (lane >= j0) & (lane < j0 + nb)
        masked = [jnp.where((lane > j0 + l) & (lane < j0 + nb), 0.0, rows[l]) for l in range(nb)]
        for t in range(t0 + tn, n // 8):
            acc = jnp.where(inside, 0.0, tiles[t])
            for l in range(nb):
                acc = acc - mult[l, t] * masked[l]
            tiles[t] = acc
        for l in range(nb):
            tl, rl = t0 + l // 8, l % 8
            tiles[tl] = jnp.where(sub == rl, tiles[tl] * lax.rsqrt(inv[l]), tiles[tl])
        for t in range(t0, t0 + tn):
            rr = sub + 8 * t
            put(t, jnp.where(lane <= rr, tiles[t], 0.0))


def factor_pair(s, inv_ref, cross_ref, w, hooks):
    def half():
        def put(t, v):
            w[8 * t : 8 * t + 8, :] = v

        eliminate(lambda t: w[8 * t : 8 * t + 8, :], put)

    for p in range(2):
        top, low = slice(p * 256, p * 256 + 128), slice(p * 256 + 128, p * 256 + 256)
        w[...] = s[top, top]
        half()
        hooks[2 * p]()
        i11 = w[...]
        l21 = dot(s[low, top], i11, 1, 1)
        w[...] = s[low, low] - dot(l21, l21, 1, 1)
        half()
        hooks[2 * p + 1]()
        i22 = w[...]
        inv_ref[p, 0:128, 0:128] = i11
        inv_ref[p, 0:128, 128:256] = jnp.zeros((128, 128), F32)
        inv_ref[p, 128:256, 128:256] = i22
        inv_ref[p, 128:256, 0:128] = -dot(i22, dot(l21, i11))
        if p == 0:
            c = dot(s[256:512, 0:256], inv_ref[0], 1, 1)
            cross_ref[...] = c
            s[256:512, 256:512] = s[256:512, 256:512] - dot(c, c, 1, 1)


def step_kernel(
    weight_ref, x_ref, out_ref, pan_ref, inv_ref, fro_ref,
    xb, other, lhs, prod, dprod, dland, dpc, dring, pland, red, pring, gpiece, gring,
    pile, turned, half_in, sqv, sqp, sqb, sqo, s, w, cross, g, low,
    s_ring, r_ring, s_core, r_core, s_drs, r_drs, s_dpl, r_dpl, s_dag, r_dag,
    s_rs, r_rs, s_ag, r_ag, s_gpl, r_gpl, s_a2a, r_a2a, s_mir, r_mir, s_sqa, r_sqa, s_sqb, r_sqb,
):
    x, y, k, z, h = place()
    a = x * 8 + y
    b = z * 2 + h

    def at_a(i):
        return (lax.div(i, 8), lax.rem(i, 8), k, z, h)

    def at_b(i):
        return (x, y, k, lax.div(i, 2), lax.rem(i, 2))

    partner = (x, y, 1 - k, z, h)
    across = (1 - x, y, k, z, h)
    mirror = (lax.div(b, 8), lax.rem(b, 8), k, lax.div(a, 2), lax.rem(a, 2))

    def copy(src, dst, ssem, rsem, dev):
        return pltpu.make_async_remote_copy(
            src_ref=src, dst_ref=dst, send_sem=ssem, recv_sem=rsem,
            device_id=dev, device_id_type=pl.DeviceIdType.MESH,
        )

    def chosen(i, j):
        odd = lax.rem(i + j, 2)
        return (i == j) | ((i < j) & (odd == 1)) | ((i > j) & (odd == 0))

    mine = chosen(a, b)

    def others(me, fn):
        @pl.loop(1, 16)
        def _(i):
            fn(i, lax.rem(me + i, 16))

    barrier = pltpu.get_barrier_semaphore()

    def signal(dev):
        pl.semaphore_signal(barrier, inc=1, device_id=dev, device_id_type=pl.DeviceIdType.MESH)

    others(a, lambda i, to: signal(at_a(to)))
    others(b, lambda i, to: signal(at_b(to)))
    signal(partner)

    @pl.when(a != b)
    def _():
        signal(mirror)

    def squares_of(v):
        return jnp.sum((v * v).reshape(64, 8, 128), axis=0)

    sqv[0] = squares_of(x_ref[...])
    xb[a] = x_ref[...]

    @pl.when(a != b)
    def _():
        pl.semaphore_wait(barrier, 32)

    @pl.when(a == b)
    def _():
        pl.semaphore_wait(barrier, 31)

    def sq_a(i, to, frm=None):
        return copy(sqv.at[0], sqp.at[a if frm is None else frm], s_sqa.at[i], r_sqa.at[a if frm is None else frm], at_a(to))

    def sq_b(i, to, frm=None):
        return copy(sqv.at[1], sqb.at[b if frm is None else frm], s_sqb.at[i], r_sqb.at[b if frm is None else frm], at_b(to))

    others(a, lambda i, to: sq_a(i, to).start())
    sqp[a] = sqv[0]

    sgn = 1 - 2 * k

    def slot(far, dy):
        return (1 - x if far else x) * 8 + lax.rem(y + dy + 8, 8)

    def y_at(dy):
        return (x, lax.rem(y + dy + 8, 8), k, z, h)

    sent = []

    def go(who, to, src=None):
        n = len(sent)
        c = copy(xb.at[who] if src is None else src, xb.at[who], s_ring.at[n], r_ring.at[who], to)
        c.start()
        sent.append(c)

    def arrive(who):
        copy(xb.at[who], xb.at[who], s_ring.at[0], r_ring.at[who], across).wait_recv()

    go(a, y_at(1), x_ref)
    go(a, y_at(-1), x_ref)
    go(a, across, x_ref)
    to_core = copy(x_ref, other, s_core.at[0], r_core.at[0], partner)
    to_core.start()

    tiles = []

    def tile(n, who):
        return copy(prod.at[who], pile.at[b], s_a2a.at[n], r_a2a.at[b], at_b(who))

    def work(far, dy):
        who = slot(far, dy)
        n = len(tiles)
        tiles.append(who)

        @pl.when(chosen(a, who) | (who < 2))
        def _():
            prod[who] = dot(xb[who], lhs[...], 0, 0)

        @pl.when(chosen(a, who) & (who != b))
        def _():
            tile(n, who).start()

    def d_rs(i, to, frm=None):
        me = b if frm is None else frm
        rows = pl.ds(pl.multiple_of(lax.rem(to, 8) * 16, 16), 16)
        return copy(dprod.at[lax.div(to, 8), rows], dland.at[me], s_drs.at[i], r_drs.at[me], at_b(to))

    def d_pl(i, to, who):
        return copy(dpc.at[who], dpc.at[who], s_dpl.at[i], r_dpl.at[who], at_a(to))

    def d_ag(i, to, frm, n):
        return copy(dpc.at[0:n], dring.at[k, frm, 0:n], s_dag.at[i], r_dag.at[frm], at_b(to))

    def p_rs(i, to, frm=None):
        me = b if frm is None else frm
        rows = pl.ds(pl.multiple_of(lax.rem(to, 8) * 16, 16), 16)
        return copy(prod.at[lax.div(to, 8), rows], pland.at[me], s_rs.at[i], r_rs.at[me], at_b(to))

    def p_ag(i, to, frm=None):
        me = b if frm is None else frm
        return copy(red, pring.at[k, me], s_ag.at[i], r_ag.at[me], at_b(to))

    def g_pl(i, to, frm=None):
        me = a if frm is None else frm
        return copy(gpiece, gring.at[k, me], s_gpl.at[i], r_gpl.at[me], at_a(to))

    def own_rows(ref):
        return ref[lax.div(b, 8), pl.ds(pl.multiple_of(lax.rem(b, 8) * 16, 16), 16), :]

    def total_of(ref):
        v = ref[0]
        for i in range(1, 16):
            v = v + ref[i]
        return v

    arrive(slot(0, -1))
    go(slot(0, -1), y_at(1))
    go(slot(0, -1), across)
    arrive(slot(0, 1))
    go(slot(0, 1), y_at(-1))
    go(slot(0, 1), across)
    to_core.wait_recv()
    lhs[:, pl.ds(pl.multiple_of(k * 128, 128), 128)] = x_ref[...]
    lhs[:, pl.ds(pl.multiple_of((1 - k) * 128, 128), 128)] = other[...]

    @pl.when(a < 2)
    def _():
        @pl.loop(0, 2)
        def _(i):
            dprod[i] = dot(xb[i], lhs[...], 0, 0)

        others(b, lambda i, to: d_rs(i, to).start())
        dland[b] = own_rows(dprod)

    others(a, lambda i, frm: sq_a(i, a, frm).wait_recv())
    sqv[1] = total_of(sqp)
    others(b, lambda i, to: sq_b(i, to).start())
    sqb[b] = sqv[1]

    work(0, 0)
    work(0, -1)
    work(0, 1)
    arrive(slot(1, 0))
    work(1, 0)
    arrive(slot(0, -2))
    go(slot(0, -2), y_at(1))
    arrive(slot(0, 2))
    go(slot(0, 2), y_at(-1))

    @pl.when(a < 2)
    def _():
        others(b, lambda i, frm: d_rs(i, frm, frm).wait_recv())
        dpc[a] = total_of(dland)

        @pl.when((a == 0) | (b >= 8))
        def _():
            others(a, lambda i, to: d_pl(i, to, a).start())

    work(0, -2)
    work(0, 2)
    arrive(slot(1, -1))
    go(slot(1, -1), y_at(1))
    arrive(slot(1, 1))
    go(slot(1, 1), y_at(-1))
    work(1, -1)
    work(1, 1)

    @pl.when(a != 0)
    def _():
        d_pl(0, 0, 0).wait_recv()

    @pl.when((a != 1) & (b >= 8))
    def _():
        d_pl(0, 1, 1).wait_recv()

    @pl.when(b < 8)
    def _():
        others(b, lambda i, to: d_ag(i, to, b, 1).start())

    @pl.when(b >= 8)
    def _():
        others(b, lambda i, to: d_ag(i, to, b, 2).start())
        dring[k, b, 1] = dpc[1]

    dring[k, b, 0] = dpc[0]
    arrive(slot(0, -3))
    arrive(slot(0, 3))
    go(slot(0, -3 * sgn), y_at(sgn))
    work(0, -3)
    work(0, 3)
    arrive(slot(1, -2))
    go(slot(1, -2), y_at(1))
    arrive(slot(1, 2))
    go(slot(1, 2), y_at(-1))
    work(1, -2)
    work(1, 2)
    arrive(slot(1, -3))
    arrive(slot(1, 3))
    go(slot(1, -3 * sgn), y_at(sgn))
    work(1, -3)
    work(1, 3)
    arrive(slot(0, 4))
    work(0, 4)
    arrive(slot(1, 4))
    work(1, 4)

    others(b, lambda i, to: p_rs(i, to).start())
    pland[b] = own_rows(prod)

    others(b, lambda i, frm: sq_b(i, b, frm).wait_recv())
    sqv[2] = total_of(sqb)
    sq_swap = copy(sqv.at[2], sqo, s_core.at[1], r_core.at[1], partner)
    sq_swap.start()

    @pl.loop(0, 8)
    def _(p):
        @pl.when(p != b)
        def _():
            d_ag(0, b, p, 1).wait_recv()

        @pl.when(p + 8 != b)
        def _():
            d_ag(0, b, p + 8, 2).wait_recv()

    d_swap = copy(dring.at[k], dring.at[k], s_core.at[2], r_core.at[2], partner)
    d_swap.start()
    sq_swap.wait_recv()
    both = sqv[2] + sqo[...]
    squares = jnp.sum(jnp.sum(both, axis=0, keepdims=True), axis=1, keepdims=True)
    fro_ref[0] = jnp.sqrt(squares)[0, 0]
    scale = weight_ref[0] / squares
    row0 = a * 256 + k * 128
    col0 = b * 256

    def iota(shape, dim, start=0):
        return lax.broadcasted_iota(jnp.int32, shape, dim) + start

    def scaled(v, r0, c0):
        eye = (iota(v.shape, 0, r0) == iota(v.shape, 1, c0)).astype(F32)
        return v * scale + eye

    copy(dring.at[1 - k], dring.at[1 - k], s_core.at[2], r_core.at[2], partner).wait_recv()
    for kk in range(2):
        for i in range(2):
            r = i * 256 + kk * 128
            for j in range(i + 1):
                v = dring[kk, 8 * i : 8 * i + 8, j].reshape(128, 256)
                s[r : r + 128, 256 * j : 256 * j + 256] = scaled(v, r, 256 * j)

    to_mirror = copy(red, gpiece, s_mir.at[0], r_mir.at[0], mirror)
    turn = copy(turned, half_in, s_mir.at[1], r_mir.at[1], mirror)
    trade = copy(
        turned.at[:, pl.ds(pl.multiple_of((1 - k) * 128, 128), 128)],
        half_in.at[:, 0:128],
        s_core.at[3], r_core.at[3], partner,
    )

    def hook_rows():
        others(b, lambda i, frm: p_rs(i, frm, frm).wait_recv())
        red[...] = total_of(pland)

        @pl.when(a != b)
        def _():
            to_mirror.start()

        others(b, lambda i, to: p_ag(i, to).start())
        pring[k, b] = red[...]

        @pl.when(a == b)
        def _():
            gpiece[...] = red[...]

    def hook_tile():
        @pl.when(mine)
        def _():
            pile[b] = prod[b]
            others(b, lambda i, frm: copy(prod.at[frm], pile.at[frm], s_a2a.at[0], r_a2a.at[frm], at_b(frm)).wait_recv())
            turned[...] = total_of(pile)
            trade.start()

            @pl.when(a != b)
            def _():
                turn.start()

    def hook_mirror():
        @pl.when(a != b)
        def _():
            to_mirror.wait_recv()

        others(a, lambda i, to: g_pl(i, to).start())
        gring[k, a] = gpiece[...]

    p_swap = copy(pring.at[k], pring.at[k], s_core.at[4], r_core.at[4], partner)
    g_swap = copy(gring.at[k], gring.at[k], s_core.at[5], r_core.at[5], partner)

    def hook_last():
        others(b, lambda i, frm: p_ag(i, b, frm).wait_recv())
        p_swap.start()

    factor_pair(s, inv_ref, cross, w, [hook_rows, hook_tile, hook_mirror, hook_last])

    others(a, lambda i, frm: g_pl(i, a, frm).wait_recv())
    g_swap.start()

    copy(pring.at[1 - k], pring.at[1 - k], s_core.at[4], r_core.at[4], partner).wait_recv()
    copy(gring.at[1 - k], gring.at[1 - k], s_core.at[5], r_core.at[5], partner).wait_recv()
    for kk in range(2):
        for i in range(2):
            r = i * 256 + kk * 128
            v = pring[kk, 8 * i : 8 * i + 8, :, pl.ds(pl.multiple_of(k * 128, 128), 128)].reshape(128, 128)
            g[r : r + 128, 0:128] = scaled(v, r, row0)
            v = gring[kk, 8 * i : 8 * i + 8].reshape(128, 256)
            g[r : r + 128, 128:384] = scaled(v, r, col0)

    lane = iota((256, 384), 1)
    ids = lane + jnp.where(lane < 128, row0, col0 - 128)
    first = iota((256, 384), 0)
    one = jnp.where(ids >= first, dot(inv_ref[0], g[0:256, :]), 0.0)
    low[0:256, :] = one
    two = dot(inv_ref[1], g[256:512, :] - dot(cross[...], one))
    low[256:512, :] = jnp.where(ids >= first + 256, two, 0.0)
    pan_ref[...] = low[:, 0:128].T
    less = dot(low[:, 0:128], low[:, 128:384], 0, 0)

    @pl.when(mine)
    def _():
        own = pl.ds(pl.multiple_of(k * 128, 128), 128)
        out_ref[:, own] = turned[:, own].T
        trade.wait_recv()
        out_ref[:, pl.ds(pl.multiple_of((1 - k) * 128, 128), 128)] = half_in[:, 0:128].T

    @pl.when(chosen(b, a) & (a != b))
    def _():
        turn.wait_recv()
        out_ref[...] = half_in[...]

    out_ref[...] = scaled(out_ref[...], row0, col0) - less

    for c in sent:
        c.wait_send()
    to_core.wait_send()
    sq_swap.wait_send()
    d_swap.wait_send()
    p_swap.wait_send()
    g_swap.wait_send()

    @pl.when(mine)
    def _():
        trade.wait_send()

    @pl.when(mine & (a != b))
    def _():
        turn.wait_send()

    @pl.when(a != b)
    def _():
        to_mirror.wait_send()

    @pl.when(a < 2)
    def _():
        others(b, lambda i, to: d_rs(i, to).wait_send())

    @pl.when((a == 0) | ((a == 1) & (b >= 8)))
    def _():
        others(a, lambda i, to: d_pl(i, to, a).wait_send())

    @pl.when(b < 8)
    def _():
        others(b, lambda i, to: d_ag(i, to, b, 1).wait_send())

    @pl.when(b >= 8)
    def _():
        others(b, lambda i, to: d_ag(i, to, b, 2).wait_send())

    others(a, lambda i, to: sq_a(i, to).wait_send())
    others(b, lambda i, to: sq_b(i, to).wait_send())
    others(b, lambda i, to: p_rs(i, to).wait_send())
    others(b, lambda i, to: p_ag(i, to).wait_send())
    others(a, lambda i, to: g_pl(i, to).wait_send())
    for n, who in enumerate(tiles):

        @pl.when(chosen(a, who) & (who != b))
        def _():
            tile(n, who).wait_send()


def on_device(x_slab, weight_c):
    vmem, smem = pl.BlockSpec(memory_space=pltpu.VMEM), pl.BlockSpec(memory_space=pltpu.SMEM)
    dma = pltpu.SemaphoreType.DMA
    shapes = [(128, 256), (128, 512), (2, 256, 256), (1,)]
    scratch = [
        (16, 512, 128), (512, 128), (512, 256), (16, 128, 256), (2, 128, 256), (16, 16, 256),
        (2, 16, 256), (2, 16, 2, 16, 256), (16, 16, 256), (16, 256), (2, 16, 16, 256), (16, 256),
        (2, 16, 16, 256), (16, 128, 256), (128, 256), (128, 256), (3, 8, 128), (16, 8, 128),
        (16, 8, 128), (8, 128), (512, 512), (128, 128), (256, 256), (512, 384), (512, 384),
    ]
    sems = [20, 16, 6, 6, 16, 16, 16, 2, 16, 16, 16, 16, 16, 16, 16, 16, 16, 16, 2, 2, 16, 16, 16, 16]
    return pl.pallas_call(
        step_kernel,
        out_shape=[jax.ShapeDtypeStruct(s, F32) for s in shapes],
        in_specs=[smem, vmem],
        out_specs=[vmem] * 3 + [smem],
        scratch_shapes=[pltpu.VMEM(s, F32) for s in scratch] + [dma((n,)) for n in sems],
        compiler_params=pltpu.CompilerParams(
            collective_id=0, has_side_effects=True, vmem_limit_bytes=48 * 1024 * 1024
        ),
        name="step",
    )(weight_c, x_slab)


def solution(mesh):
    split = Mesh(mesh.devices.reshape(2, 8, 2, 8, 2), AXES)
    return jax.shard_map(
        on_device, mesh=split, in_specs=(P(COL, ROW), P()),
        out_specs=(P(ROW, COL), P(ROW, None), P(), P()), check_vma=False,
    )
```

```python
import jax
import jax.numpy as jnp
from jax import lax
from jax.experimental import pallas as pl
from jax.experimental.pallas import tpu as pltpu
from jax.sharding import Mesh
from jax.sharding import PartitionSpec as P

AXES = ("x", "y", "core", "z", "h")
ROW = ("x", "y", "core")
COL = ("z", "h")
HIGH = lax.Precision.HIGHEST
F32 = jnp.float32


def place():
    x, y, k = lax.axis_index("x"), lax.axis_index("y"), lax.axis_index("core")
    z, h = lax.axis_index("z"), lax.axis_index("h")
    return x, y, k, z, h


def dot(left, right, ca=1, cb=0):
    return lax.dot_general(
        left, right, (((ca,), (cb,)), ((), ())), precision=HIGH, preferred_element_type=F32
    )


def eliminate(get, put, mid, n=128, nb=8):
    lane = lax.broadcasted_iota(jnp.int32, (8, n), 1)
    sub = lax.broadcasted_iota(jnp.int32, (8, n), 0)
    tiles = [get(t) for t in range(n // 8)]
    for j0 in range(0, n, nb):
        if j0 == 64:
            mid()
        t0 = j0 // 8
        tn = nb // 8
        live = range(t0, n // 8)
        cols = {}
        for l in range(nb):
            for t in live:
                cols[l, t] = jnp.broadcast_to(tiles[t][:, j0 + l : j0 + l + 1], (8, n))
        mult = {}
        inv = []
        for l in range(nb):
            tl, rl = t0 + l // 8, l % 8
            piv = jnp.broadcast_to(cols[l, tl][rl : rl + 1, :], (8, n))
            r = 1.0 / piv
            inv.append(piv)
            for t in live:
                if t < tl:
                    continue
                m = cols[l, t] * r
                if t == tl:
                    m = jnp.where(sub > rl, m, 0.0)
                mult[l, t] = m
            for q in range(l + 1, nb):
                tq, rq = t0 + q // 8, q % 8
                s = jnp.broadcast_to(cols[l, tq][rq : rq + 1, :], (8, n))
                for t in live:
                    if t < tq:
                        continue
                    cols[q, t] = cols[q, t] - mult[l, t] * s
        rows = []
        for l in range(nb):
            tl, rl = t0 + l // 8, l % 8
            piv_row = jnp.where(lane == j0 + l, 1.0, jnp.broadcast_to(tiles[tl][rl : rl + 1, :], (8, n)))
            rows.append(piv_row)
            for t in range(tl, t0 + tn):
                keep = tiles[t]
                if t == tl:
                    zeroed = jnp.where((lane == j0 + l) & (sub > rl), 0.0, keep)
                    tiles[t] = zeroed - mult[l, t] * piv_row
                else:
                    tiles[t] = jnp.where(lane == j0 + l, 0.0, keep) - mult[l, t] * piv_row
            tiles[tl] = jnp.where((sub == rl), piv_row, tiles[tl])
        inside = (lane >= j0) & (lane < j0 + nb)
        masked = [jnp.where((lane > j0 + l) & (lane < j0 + nb), 0.0, rows[l]) for l in range(nb)]
        for t in range(t0 + tn, n // 8):
            acc = jnp.where(inside, 0.0, tiles[t])
            for l in range(nb):
                acc = acc - mult[l, t] * masked[l]
            tiles[t] = acc
        for l in range(nb):
            tl, rl = t0 + l // 8, l % 8
            tiles[tl] = jnp.where(sub == rl, tiles[tl] * lax.rsqrt(inv[l]), tiles[tl])
        for t in range(t0, t0 + tn):
            rr = sub + 8 * t
            put(t, jnp.where(lane <= rr, tiles[t], 0.0))


def factor_pair(s, inv_ref, cross_ref, w, hooks):
    def half(mid):
        def put(t, v):
            w[8 * t : 8 * t + 8, :] = v

        eliminate(lambda t: w[8 * t : 8 * t + 8, :], put, mid)

    for p in range(2):
        top, low = slice(p * 256, p * 256 + 128), slice(p * 256 + 128, p * 256 + 256)
        w[...] = s[top, top]
        half(hooks[4 * p])
        hooks[4 * p + 1]()
        i11 = w[...]
        l21 = dot(s[low, top], i11, 1, 1)
        w[...] = s[low, low] - dot(l21, l21, 1, 1)
        half(hooks[4 * p + 2])
        hooks[4 * p + 3]()
        i22 = w[...]
        inv_ref[p, 0:128, 0:128] = i11
        inv_ref[p, 0:128, 128:256] = jnp.zeros((128, 128), F32)
        inv_ref[p, 128:256, 128:256] = i22
        inv_ref[p, 128:256, 0:128] = -dot(i22, dot(l21, i11))
        if p == 0:
            c = dot(s[256:512, 0:256], inv_ref[0], 1, 1)
            cross_ref[...] = c
            s[256:512, 256:512] = s[256:512, 256:512] - dot(c, c, 1, 1)


def step_kernel(
    weight_ref, x_ref, out_ref, pan_ref, inv_ref, fro_ref,
    xb, other, lhs, prod, dprod, dland, dpc, dring, pland, red, pring, gpiece, gring,
    pile, part, hland, turned, half_in, sqv, sqp, sqb, sqo, s, w, cross, g, low,
    s_ring, r_ring, s_core, r_core, s_drs, r_drs, s_dpl, r_dpl, s_dag, r_dag,
    s_rs, r_rs, s_ag, r_ag, s_gpl, r_gpl, s_a2a, r_a2a, s_h, r_h, s_mir, r_mir, s_sqa, r_sqa, s_sqb, r_sqb,
):
    x, y, k, z, h = place()
    a = x * 8 + y
    b = z * 2 + h

    def at_a(i):
        return (lax.div(i, 8), lax.rem(i, 8), k, z, h)

    def at_b(i):
        return (x, y, k, lax.div(i, 2), lax.rem(i, 2))

    partner = (x, y, 1 - k, z, h)
    across = (1 - x, y, k, z, h)
    mirror = (lax.div(b, 8), lax.rem(b, 8), k, lax.div(a, 2), lax.rem(a, 2))

    def copy(src, dst, ssem, rsem, dev):
        return pltpu.make_async_remote_copy(
            src_ref=src, dst_ref=dst, send_sem=ssem, recv_sem=rsem,
            device_id=dev, device_id_type=pl.DeviceIdType.MESH,
        )

    def chosen(i, j):
        odd = lax.rem(i + j, 2)
        return (i == j) | ((i < j) & (odd == 1)) | ((i > j) & (odd == 0))

    mine = chosen(a, b)
    twin = z * 2 + 1 - h
    helps = chosen(a, twin)

    def others(me, fn):
        @pl.loop(1, 16)
        def _(i):
            fn(i, lax.rem(me + i, 16))

    barrier = pltpu.get_barrier_semaphore()

    def signal(dev):
        pl.semaphore_signal(barrier, inc=1, device_id=dev, device_id_type=pl.DeviceIdType.MESH)

    others(a, lambda i, to: signal(at_a(to)))
    others(b, lambda i, to: signal(at_b(to)))
    signal(partner)

    @pl.when(a != b)
    def _():
        signal(mirror)

    def squares_of(v):
        return jnp.sum((v * v).reshape(64, 8, 128), axis=0)

    sqv[0] = squares_of(x_ref[...])
    xb[a] = x_ref[...]

    @pl.when(a != b)
    def _():
        pl.semaphore_wait(barrier, 32)

    @pl.when(a == b)
    def _():
        pl.semaphore_wait(barrier, 31)

    def sq_a(i, to, frm=None):
        return copy(sqv.at[0], sqp.at[a if frm is None else frm], s_sqa.at[i], r_sqa.at[a if frm is None else frm], at_a(to))

    def sq_b(i, to, frm=None):
        return copy(sqv.at[1], sqb.at[b if frm is None else frm], s_sqb.at[i], r_sqb.at[b if frm is None else frm], at_b(to))

    others(a, lambda i, to: sq_a(i, to).start())
    sqp[a] = sqv[0]

    sgn = 1 - 2 * k

    def slot(far, dy):
        return (1 - x if far else x) * 8 + lax.rem(y + dy + 8, 8)

    def y_at(dy):
        return (x, lax.rem(y + dy + 8, 8), k, z, h)

    sent = []

    def part_of(ref, c):
        return ref.at[256 * c : 256 * c + 256]

    def go(who, c, to, src=None):
        n = len(sent)
        dst = part_of(xb.at[who], c)
        d = copy(dst if src is None else part_of(src, c), dst, s_ring.at[n], r_ring.at[2 * who + c], to)
        d.start()
        sent.append(d)

    def arrive(who, c):
        dst = part_of(xb.at[who], c)
        copy(dst, dst, s_ring.at[0], r_ring.at[2 * who + c], across).wait_recv()

    def onward(far, dy, c, to_x=False, to_y=True):
        for sign in (-1, 1):
            who = slot(far, sign * dy)
            arrive(who, c)
            if to_y:
                go(who, c, y_at(-sign))
            if to_x:
                go(who, c, across)

    def last_hop(far, c):
        arrive(slot(far, -3), c)
        arrive(slot(far, 3), c)
        go(slot(far, -3 * sgn), c, y_at(sgn))

    for c in range(2):
        go(a, c, y_at(1), x_ref)
        go(a, c, y_at(-1), x_ref)
        go(a, c, across, x_ref)
    to_core = copy(x_ref, other, s_core.at[0], r_core.at[0], partner)
    to_core.start()

    tiles = []

    def tile(n, who):
        dest, side = lax.div(who, 2), lax.rem(who, 2)
        return copy(
            prod.at[who], pile.at[side, z], s_a2a.at[n], r_a2a.at[side * 8 + z], (x, y, k, dest, h)
        )

    held = []

    def ship(n, who):
        @pl.when(chosen(a, who) & (lax.div(who, 2) != z))
        def _():
            tile(n, who).start()

    def work(far, dy, hold=False):
        who = slot(far, dy)
        n = len(tiles)
        tiles.append(who)

        @pl.when(chosen(a, who) | (who < 2))
        def _():
            prod[who] = dot(xb[who], lhs[...], 0, 0)

        if hold:
            held.append((n, who))
        else:
            ship(n, who)

    def d_rs(i, to, frm=None):
        me = b if frm is None else frm
        rows = pl.ds(pl.multiple_of(lax.rem(to, 8) * 16, 16), 16)
        return copy(dprod.at[lax.div(to, 8), rows], dland.at[me], s_drs.at[i], r_drs.at[me], at_b(to))

    def d_pl(i, to, who):
        return copy(dpc.at[who], dpc.at[who], s_dpl.at[i], r_dpl.at[who], at_a(to))

    def d_ag(i, to, frm, n):
        return copy(dpc.at[0:n], dring.at[k, frm, 0:n], s_dag.at[i], r_dag.at[frm], at_b(to))

    def p_rs(i, to, frm=None):
        me = b if frm is None else frm
        rows = pl.ds(pl.multiple_of(lax.rem(to, 8) * 16, 16), 16)
        return copy(prod.at[lax.div(to, 8), rows], pland.at[me], s_rs.at[i], r_rs.at[me], at_b(to))

    def p_ag(i, to, frm=None):
        me = b if frm is None else frm
        return copy(red, pring.at[k, me], s_ag.at[i], r_ag.at[me], at_b(to))

    def g_pl(i, to, frm=None):
        me = a if frm is None else frm
        return copy(gpiece, gring.at[k, me], s_gpl.at[i], r_gpl.at[me], at_a(to))

    def own_rows(ref):
        return ref[lax.div(b, 8), pl.ds(pl.multiple_of(lax.rem(b, 8) * 16, 16), 16), :]

    def total_of(ref):
        v = ref[0]
        for i in range(1, 16):
            v = v + ref[i]
        return v

    onward(0, 1, 0, to_x=True)
    onward(0, 1, 1, to_x=True)
    to_core.wait_recv()
    lhs[:, pl.ds(pl.multiple_of(k * 128, 128), 128)] = x_ref[...]
    lhs[:, pl.ds(pl.multiple_of((1 - k) * 128, 128), 128)] = other[...]

    @pl.when(a < 2)
    def _():
        @pl.loop(0, 2)
        def _(i):
            dprod[i] = dot(xb[i], lhs[...], 0, 0)

        others(b, lambda i, to: d_rs(i, to).start())
        dland[b] = own_rows(dprod)

    others(a, lambda i, frm: sq_a(i, a, frm).wait_recv())
    sqv[1] = total_of(sqp)
    others(b, lambda i, to: sq_b(i, to).start())
    sqb[b] = sqv[1]

    work(0, 0)
    work(0, -1)
    work(0, 1)
    onward(0, 2, 0, to_x=True)
    arrive(slot(1, 0), 0)
    arrive(slot(1, 0), 1)
    onward(0, 2, 1)
    work(1, 0)
    work(0, -2)
    work(0, 2)
    onward(1, 1, 0, to_y=False)
    onward(1, 1, 1)
    work(1, -1)
    work(1, 1)
    last_hop(0, 0)
    last_hop(0, 1)
    @pl.when(a < 2)
    def _():
        others(b, lambda i, frm: d_rs(i, frm, frm).wait_recv())
        dpc[a] = total_of(dland)

        @pl.when((a == 0) | (b >= 8))
        def _():
            others(a, lambda i, to: d_pl(i, to, a).start())

    work(0, -3, True)
    work(0, 3, True)
    onward(1, 2, 0)
    onward(1, 2, 1)
    work(1, -2, True)
    work(1, 2, True)
    last_hop(1, 0)
    last_hop(1, 1)
    @pl.when(a != 0)
    def _():
        d_pl(0, 0, 0).wait_recv()

    @pl.when((a != 1) & (b >= 8))
    def _():
        d_pl(0, 1, 1).wait_recv()

    @pl.when(b < 8)
    def _():
        others(b, lambda i, to: d_ag(i, to, b, 1).start())

    @pl.when(b >= 8)
    def _():
        others(b, lambda i, to: d_ag(i, to, b, 2).start())
        dring[k, b, 1] = dpc[1]

    dring[k, b, 0] = dpc[0]
    arrive(slot(0, 4), 0)
    arrive(slot(0, 4), 1)
    work(0, 4, True)
    work(1, -3, True)
    work(1, 3, True)
    arrive(slot(1, 4), 0)
    arrive(slot(1, 4), 1)
    work(1, 4, True)

    others(b, lambda i, to: p_rs(i, to).start())
    pland[b] = own_rows(prod)
    for n, who in held:
        ship(n, who)

    others(b, lambda i, frm: sq_b(i, b, frm).wait_recv())
    sqv[2] = total_of(sqb)
    sq_swap = copy(sqv.at[2], sqo, s_core.at[1], r_core.at[1], partner)
    sq_swap.start()

    @pl.loop(0, 8)
    def _(p):
        @pl.when(p != b)
        def _():
            d_ag(0, b, p, 1).wait_recv()

        @pl.when(p + 8 != b)
        def _():
            d_ag(0, b, p + 8, 2).wait_recv()

    d_swap = copy(dring.at[k], dring.at[k], s_core.at[2], r_core.at[2], partner)
    d_swap.start()
    sq_swap.wait_recv()
    both = sqv[2] + sqo[...]
    squares = jnp.sum(jnp.sum(both, axis=0, keepdims=True), axis=1, keepdims=True)
    fro_ref[0] = jnp.sqrt(squares)[0, 0]
    scale = weight_ref[0] / squares
    row0 = a * 256 + k * 128
    col0 = b * 256

    def iota(shape, dim, start=0):
        return lax.broadcasted_iota(jnp.int32, shape, dim) + start

    def scaled(v, r0, c0):
        eye = (iota(v.shape, 0, r0) == iota(v.shape, 1, c0)).astype(F32)
        return v * scale + eye

    copy(dring.at[1 - k], dring.at[1 - k], s_core.at[2], r_core.at[2], partner).wait_recv()
    for kk in range(2):
        for i in range(2):
            r = i * 256 + kk * 128
            for j in range(i + 1):
                v = dring[kk, 8 * i : 8 * i + 8, j].reshape(128, 256)
                s[r : r + 128, 256 * j : 256 * j + 256] = scaled(v, r, 256 * j)

    to_mirror = copy(red, gpiece, s_mir.at[0], r_mir.at[0], mirror)
    turn = copy(turned, half_in, s_mir.at[1], r_mir.at[1], mirror)
    trade = copy(
        turned.at[:, pl.ds(pl.multiple_of((1 - k) * 128, 128), 128)],
        half_in.at[:, 0:128],
        s_core.at[3], r_core.at[3], partner,
    )

    def hook_rows():
        others(b, lambda i, frm: p_rs(i, frm, frm).wait_recv())
        red[...] = total_of(pland)

        @pl.when(a != b)
        def _():
            to_mirror.start()

        others(b, lambda i, to: p_ag(i, to).start())
        pring[k, b] = red[...]

        @pl.when(a == b)
        def _():
            gpiece[...] = red[...]

    to_twin = copy(part, hland, s_h.at[0], r_h.at[0], (x, y, k, z, 1 - h))

    def sum_over_z(side, who):
        pile[side, z] = prod[who]

        @pl.loop(1, 8)
        def _(i):
            frm = lax.rem(z + i, 8)
            copy(
                prod.at[who], pile.at[side, frm], s_a2a.at[0], r_a2a.at[side * 8 + frm],
                (x, y, k, frm, h),
            ).wait_recv()

        v = pile[side, 0]
        for i in range(1, 8):
            v = v + pile[side, i]
        return v

    def hook_half():
        @pl.when(helps)
        def _():
            part[...] = sum_over_z(1 - h, twin)
            to_twin.start()

        @pl.when(mine)
        def _():
            turned[...] = sum_over_z(h, b)

    def hook_tile():
        @pl.when(mine)
        def _():
            to_twin.wait_recv()
            turned[...] = turned[...] + hland[...]
            trade.start()

            @pl.when(a != b)
            def _():
                turn.start()

    def hook_mirror():
        @pl.when(a != b)
        def _():
            to_mirror.wait_recv()

        others(a, lambda i, to: g_pl(i, to).start())
        gring[k, a] = gpiece[...]

    p_swap = copy(pring.at[k], pring.at[k], s_core.at[4], r_core.at[4], partner)
    g_swap = copy(gring.at[k], gring.at[k], s_core.at[5], r_core.at[5], partner)

    def hook_last():
        others(b, lambda i, frm: p_ag(i, b, frm).wait_recv())
        p_swap.start()

    def hook_rest():
        others(a, lambda i, frm: g_pl(i, a, frm).wait_recv())
        g_swap.start()

    def idle():
        pass

    factor_pair(
        s, inv_ref, cross, w,
        [idle, idle, hook_rows, hook_half, hook_mirror, hook_tile, hook_last, hook_rest],
    )

    copy(pring.at[1 - k], pring.at[1 - k], s_core.at[4], r_core.at[4], partner).wait_recv()
    copy(gring.at[1 - k], gring.at[1 - k], s_core.at[5], r_core.at[5], partner).wait_recv()
    for kk in range(2):
        for i in range(2):
            r = i * 256 + kk * 128
            v = pring[kk, 8 * i : 8 * i + 8, :, pl.ds(pl.multiple_of(k * 128, 128), 128)].reshape(128, 128)
            g[r : r + 128, 0:128] = scaled(v, r, row0)
            v = gring[kk, 8 * i : 8 * i + 8].reshape(128, 256)
            g[r : r + 128, 128:384] = scaled(v, r, col0)

    lane = iota((256, 384), 1)
    ids = lane + jnp.where(lane < 128, row0, col0 - 128)
    first = iota((256, 384), 0)
    one = jnp.where(ids >= first, dot(inv_ref[0], g[0:256, :]), 0.0)
    low[0:256, :] = one
    two = dot(inv_ref[1], g[256:512, :] - dot(cross[...], one))
    low[256:512, :] = jnp.where(ids >= first + 256, two, 0.0)
    pan_ref[...] = low[:, 0:128].T
    less = dot(low[:, 0:128], low[:, 128:384], 0, 0)

    @pl.when(mine)
    def _():
        own = pl.ds(pl.multiple_of(k * 128, 128), 128)
        out_ref[:, own] = turned[:, own].T
        trade.wait_recv()
        out_ref[:, pl.ds(pl.multiple_of((1 - k) * 128, 128), 128)] = half_in[:, 0:128].T

    @pl.when(chosen(b, a) & (a != b))
    def _():
        turn.wait_recv()
        out_ref[...] = half_in[...]

    out_ref[...] = scaled(out_ref[...], row0, col0) - less

    for c in sent:
        c.wait_send()
    to_core.wait_send()
    sq_swap.wait_send()
    d_swap.wait_send()
    p_swap.wait_send()
    g_swap.wait_send()

    @pl.when(mine)
    def _():
        trade.wait_send()

    @pl.when(mine & (a != b))
    def _():
        turn.wait_send()

    @pl.when(helps)
    def _():
        to_twin.wait_send()

    @pl.when(a != b)
    def _():
        to_mirror.wait_send()

    @pl.when(a < 2)
    def _():
        others(b, lambda i, to: d_rs(i, to).wait_send())

    @pl.when((a == 0) | ((a == 1) & (b >= 8)))
    def _():
        others(a, lambda i, to: d_pl(i, to, a).wait_send())

    @pl.when(b < 8)
    def _():
        others(b, lambda i, to: d_ag(i, to, b, 1).wait_send())

    @pl.when(b >= 8)
    def _():
        others(b, lambda i, to: d_ag(i, to, b, 2).wait_send())

    others(a, lambda i, to: sq_a(i, to).wait_send())
    others(b, lambda i, to: sq_b(i, to).wait_send())
    others(b, lambda i, to: p_rs(i, to).wait_send())
    others(b, lambda i, to: p_ag(i, to).wait_send())
    others(a, lambda i, to: g_pl(i, to).wait_send())
    for n, who in enumerate(tiles):

        @pl.when(chosen(a, who) & (lax.div(who, 2) != z))
        def _():
            tile(n, who).wait_send()


def on_device(x_slab, weight_c):
    vmem, smem = pl.BlockSpec(memory_space=pltpu.VMEM), pl.BlockSpec(memory_space=pltpu.SMEM)
    dma = pltpu.SemaphoreType.DMA
    shapes = [(128, 256), (128, 512), (2, 256, 256), (1,)]
    scratch = [
        (16, 512, 128), (512, 128), (512, 256), (16, 128, 256), (2, 128, 256), (16, 16, 256),
        (2, 16, 256), (2, 16, 2, 16, 256), (16, 16, 256), (16, 256), (2, 16, 16, 256), (16, 256),
        (2, 16, 16, 256), (2, 8, 128, 256), (128, 256), (128, 256), (128, 256), (128, 256), (3, 8, 128), (16, 8, 128),
        (16, 8, 128), (8, 128), (512, 512), (128, 128), (256, 256), (512, 384), (512, 384),
    ]
    sems = [40, 32, 6, 6, 16, 16, 16, 2, 16, 16, 16, 16, 16, 16, 16, 16, 16, 16, 1, 1, 2, 2, 16, 16, 16, 16]
    return pl.pallas_call(
        step_kernel,
        out_shape=[jax.ShapeDtypeStruct(s, F32) for s in shapes],
        in_specs=[smem, vmem],
        out_specs=[vmem] * 3 + [smem],
        scratch_shapes=[pltpu.VMEM(s, F32) for s in scratch] + [dma((n,)) for n in sems],
        compiler_params=pltpu.CompilerParams(
            collective_id=0, has_side_effects=True, vmem_limit_bytes=48 * 1024 * 1024
        ),
        name="step",
    )(weight_c, x_slab)


def solution(mesh):
    split = Mesh(mesh.devices.reshape(2, 8, 2, 8, 2), AXES)
    return jax.shard_map(
        on_device, mesh=split, in_specs=(P(COL, ROW), P()),
        out_specs=(P(ROW, COL), P(ROW, None), P(), P()), check_vma=False,
    )
```

```python
import jax
import jax.numpy as jnp
from jax import lax
from jax.experimental import pallas as pl
from jax.experimental.pallas import tpu as pltpu
from jax.sharding import Mesh
from jax.sharding import PartitionSpec as P

AXES = ("x", "y", "core", "z", "h")
ROW = ("x", "y", "core")
COL = ("z", "h")
HIGH = lax.Precision.HIGHEST
F32 = jnp.float32


def place():
    x, y, k = lax.axis_index("x"), lax.axis_index("y"), lax.axis_index("core")
    z, h = lax.axis_index("z"), lax.axis_index("h")
    return x, y, k, z, h


def dot(left, right, ca=1, cb=0):
    return lax.dot_general(
        left, right, (((ca,), (cb,)), ((), ())), precision=HIGH, preferred_element_type=F32
    )


def eliminate(get, put, mid, n=128, nb=8):
    lane = lax.broadcasted_iota(jnp.int32, (8, n), 1)
    sub = lax.broadcasted_iota(jnp.int32, (8, n), 0)
    tiles = [get(t) for t in range(n // 8)]
    for j0 in range(0, n, nb):
        if j0 == 64:
            mid()
        t0 = j0 // 8
        tn = nb // 8
        live = range(t0, n // 8)
        cols = {}
        for l in range(nb):
            for t in live:
                cols[l, t] = jnp.broadcast_to(tiles[t][:, j0 + l : j0 + l + 1], (8, n))
        mult = {}
        inv = []
        for l in range(nb):
            tl, rl = t0 + l // 8, l % 8
            piv = jnp.broadcast_to(cols[l, tl][rl : rl + 1, :], (8, n))
            r = 1.0 / piv
            inv.append(piv)
            for t in live:
                if t < tl:
                    continue
                m = cols[l, t] * r
                if t == tl:
                    m = jnp.where(sub > rl, m, 0.0)
                mult[l, t] = m
            for q in range(l + 1, nb):
                tq, rq = t0 + q // 8, q % 8
                s = jnp.broadcast_to(cols[l, tq][rq : rq + 1, :], (8, n))
                for t in live:
                    if t < tq:
                        continue
                    cols[q, t] = cols[q, t] - mult[l, t] * s
        rows = []
        for l in range(nb):
            tl, rl = t0 + l // 8, l % 8
            piv_row = jnp.where(lane == j0 + l, 1.0, jnp.broadcast_to(tiles[tl][rl : rl + 1, :], (8, n)))
            rows.append(piv_row)
            for t in range(tl, t0 + tn):
                keep = tiles[t]
                if t == tl:
                    zeroed = jnp.where((lane == j0 + l) & (sub > rl), 0.0, keep)
                    tiles[t] = zeroed - mult[l, t] * piv_row
                else:
                    tiles[t] = jnp.where(lane == j0 + l, 0.0, keep) - mult[l, t] * piv_row
            tiles[tl] = jnp.where((sub == rl), piv_row, tiles[tl])
        inside = (lane >= j0) & (lane < j0 + nb)
        masked = [jnp.where((lane > j0 + l) & (lane < j0 + nb), 0.0, rows[l]) for l in range(nb)]
        for t in range(t0 + tn, n // 8):
            acc = jnp.where(inside, 0.0, tiles[t])
            for l in range(nb):
                acc = acc - mult[l, t] * masked[l]
            tiles[t] = acc
        for l in range(nb):
            tl, rl = t0 + l // 8, l % 8
            tiles[tl] = jnp.where(sub == rl, tiles[tl] * lax.rsqrt(inv[l]), tiles[tl])
        for t in range(t0, t0 + tn):
            rr = sub + 8 * t
            put(t, jnp.where(lane <= rr, tiles[t], 0.0))


def factor_pair(s, inv_ref, cross_ref, w, hooks):
    def half(mid):
        def put(t, v):
            w[8 * t : 8 * t + 8, :] = v

        eliminate(lambda t: w[8 * t : 8 * t + 8, :], put, mid)

    for p in range(2):
        top, low = slice(p * 256, p * 256 + 128), slice(p * 256 + 128, p * 256 + 256)
        w[...] = s[top, top]
        half(hooks[4 * p])
        hooks[4 * p + 1]()
        i11 = w[...]
        l21 = dot(s[low, top], i11, 1, 1)
        w[...] = s[low, low] - dot(l21, l21, 1, 1)
        half(hooks[4 * p + 2])
        hooks[4 * p + 3]()
        i22 = w[...]
        inv_ref[p, 0:128, 0:128] = i11
        inv_ref[p, 0:128, 128:256] = jnp.zeros((128, 128), F32)
        inv_ref[p, 128:256, 128:256] = i22
        inv_ref[p, 128:256, 0:128] = -dot(i22, dot(l21, i11))
        if p == 0:
            c = dot(s[256:512, 0:256], inv_ref[0], 1, 1)
            cross_ref[...] = c
            s[256:512, 256:512] = s[256:512, 256:512] - dot(c, c, 1, 1)


def step_kernel(
    weight_ref, x_ref, out_ref, pan_ref, inv_ref, fro_ref,
    xb, other, lhs, prod, dprod, dland, dpc, dring, pland, red, pring, gpiece, gring,
    pile, part, hland, turned, half_in, sqv, sqp, sqb, sqo, s, w, cross, g, low,
    s_ring, r_ring, s_core, r_core, s_drs, r_drs, s_dpl, r_dpl, s_dag, r_dag,
    s_rs, r_rs, s_ag, r_ag, s_gpl, r_gpl, s_a2a, r_a2a, s_h, r_h, s_mir, r_mir, s_sqa, r_sqa, s_sqb, r_sqb,
):
    x, y, k, z, h = place()
    a = x * 8 + y
    b = z * 2 + h

    def at_a(i):
        return (lax.div(i, 8), lax.rem(i, 8), k, z, h)

    def at_b(i):
        return (x, y, k, lax.div(i, 2), lax.rem(i, 2))

    partner = (x, y, 1 - k, z, h)
    across = (1 - x, y, k, z, h)
    mirror = (lax.div(b, 8), lax.rem(b, 8), k, lax.div(a, 2), lax.rem(a, 2))

    def copy(src, dst, ssem, rsem, dev):
        return pltpu.make_async_remote_copy(
            src_ref=src, dst_ref=dst, send_sem=ssem, recv_sem=rsem,
            device_id=dev, device_id_type=pl.DeviceIdType.MESH,
        )

    def chosen(i, j):
        odd = lax.rem(i + j, 2)
        return (i == j) | ((i < j) & (odd == 1)) | ((i > j) & (odd == 0))

    mine = chosen(a, b)
    twin = z * 2 + 1 - h
    helps = chosen(a, twin)

    def others(me, fn):
        @pl.loop(1, 16)
        def _(i):
            fn(i, lax.rem(me + i, 16))

    barrier = pltpu.get_barrier_semaphore()

    def signal(dev):
        pl.semaphore_signal(barrier, inc=1, device_id=dev, device_id_type=pl.DeviceIdType.MESH)

    others(a, lambda i, to: signal(at_a(to)))
    others(b, lambda i, to: signal(at_b(to)))
    signal(partner)

    @pl.when(a != b)
    def _():
        signal(mirror)

    def squares_of(v):
        return jnp.sum((v * v).reshape(64, 8, 128), axis=0)

    sqv[0] = squares_of(x_ref[...])
    xb[a] = x_ref[...]

    @pl.when(a != b)
    def _():
        pl.semaphore_wait(barrier, 32)

    @pl.when(a == b)
    def _():
        pl.semaphore_wait(barrier, 31)

    def sq_a(i, to, frm=None):
        return copy(sqv.at[0], sqp.at[a if frm is None else frm], s_sqa.at[i], r_sqa.at[a if frm is None else frm], at_a(to))

    def sq_b(i, to, frm=None):
        return copy(sqv.at[1], sqb.at[b if frm is None else frm], s_sqb.at[i], r_sqb.at[b if frm is None else frm], at_b(to))

    others(a, lambda i, to: sq_a(i, to).start())
    sqp[a] = sqv[0]

    sgn = 1 - 2 * k

    def slot(far, dy):
        return (1 - x if far else x) * 8 + lax.rem(y + dy + 8, 8)

    def y_at(dy):
        return (x, lax.rem(y + dy + 8, 8), k, z, h)

    sent = []

    def part_of(ref, c):
        return ref.at[256 * c : 256 * c + 256]

    def go(who, c, to, src=None):
        n = len(sent)
        dst = part_of(xb.at[who], c)
        d = copy(dst if src is None else part_of(src, c), dst, s_ring.at[n], r_ring.at[2 * who + c], to)
        d.start()
        sent.append(d)

    def arrive(who, c):
        dst = part_of(xb.at[who], c)
        copy(dst, dst, s_ring.at[0], r_ring.at[2 * who + c], across).wait_recv()

    def onward(far, dy, c, to_x=False, to_y=True):
        for sign in (-1, 1):
            who = slot(far, sign * dy)
            arrive(who, c)
            if to_y:
                go(who, c, y_at(-sign))
            if to_x:
                go(who, c, across)

    def last_hop(far, c):
        arrive(slot(far, -3), c)
        arrive(slot(far, 3), c)
        go(slot(far, -3 * sgn), c, y_at(sgn))

    for c in range(2):
        go(a, c, y_at(1), x_ref)
        go(a, c, y_at(-1), x_ref)
        go(a, c, across, x_ref)
    to_core = copy(x_ref, other, s_core.at[0], r_core.at[0], partner)
    to_core.start()

    tiles = []

    def tile(n, who):
        dest, side = lax.div(who, 2), lax.rem(who, 2)
        return copy(
            prod.at[who], pile.at[side, z], s_a2a.at[n], r_a2a.at[side * 8 + z], (x, y, k, dest, h)
        )

    held = []

    def ship(n, who):
        @pl.when(chosen(a, who) & (lax.div(who, 2) != z))
        def _():
            tile(n, who).start()

    def multiply(n, who):
        @pl.when(chosen(a, who))
        def _():
            prod[who] = dot(xb[who], lhs[...], 0, 0)

        ship(n, who)

    def work(far, dy, hold=False):
        who = slot(far, dy)
        n = len(tiles)
        tiles.append(who)
        if hold:
            held.append((n, who))
        else:
            multiply(n, who)

    def d_rs(i, to, frm=None):
        me = b if frm is None else frm
        rows = pl.ds(pl.multiple_of(lax.rem(to, 8) * 16, 16), 16)
        return copy(dprod.at[lax.div(to, 8), rows], dland.at[me], s_drs.at[i], r_drs.at[me], at_b(to))

    def d_pl(i, to, who):
        return copy(dpc.at[who], dpc.at[who], s_dpl.at[i], r_dpl.at[who], at_a(to))

    def d_ag(i, to, frm, n):
        return copy(dpc.at[0:n], dring.at[k, frm, 0:n], s_dag.at[i], r_dag.at[frm], at_b(to))

    def p_rs(i, to, frm=None):
        me = b if frm is None else frm
        rows = pl.ds(pl.multiple_of(lax.rem(to, 8) * 16, 16), 16)
        return copy(dprod.at[lax.div(to, 8), rows], pland.at[me], s_rs.at[i], r_rs.at[me], at_b(to))

    def p_ag(i, to, frm=None):
        me = b if frm is None else frm
        return copy(red, pring.at[k, me], s_ag.at[i], r_ag.at[me], at_b(to))

    def g_pl(i, to, frm=None):
        me = a if frm is None else frm
        return copy(gpiece, gring.at[k, me], s_gpl.at[i], r_gpl.at[me], at_a(to))

    def own_rows(ref):
        return ref[lax.div(b, 8), pl.ds(pl.multiple_of(lax.rem(b, 8) * 16, 16), 16), :]

    def total_of(ref):
        v = ref[0]
        for i in range(1, 16):
            v = v + ref[i]
        return v

    onward(0, 1, 0, to_x=True)
    onward(0, 1, 1, to_x=True)
    to_core.wait_recv()
    lhs[:, pl.ds(pl.multiple_of(k * 128, 128), 128)] = x_ref[...]
    lhs[:, pl.ds(pl.multiple_of((1 - k) * 128, 128), 128)] = other[...]

    @pl.when(a < 2)
    def _():
        @pl.loop(0, 2)
        def _(i):
            dprod[i] = dot(xb[i], lhs[...], 0, 0)

        others(b, lambda i, to: d_rs(i, to).start())
        dland[b] = own_rows(dprod)

    others(a, lambda i, frm: sq_a(i, a, frm).wait_recv())
    sqv[1] = total_of(sqp)
    others(b, lambda i, to: sq_b(i, to).start())
    sqb[b] = sqv[1]

    work(0, 0)
    work(0, -1)
    work(0, 1)
    onward(0, 2, 0, to_x=True)
    arrive(slot(1, 0), 0)
    arrive(slot(1, 0), 1)
    onward(0, 2, 1)
    work(1, 0)
    work(0, -2)
    work(0, 2)
    onward(1, 1, 0, to_y=False)
    onward(1, 1, 1)
    work(1, -1)
    work(1, 1)
    last_hop(0, 0)
    last_hop(0, 1)
    @pl.when(a < 2)
    def _():
        others(b, lambda i, frm: d_rs(i, frm, frm).wait_recv())
        dpc[a] = total_of(dland)

        @pl.when((a == 0) | (b >= 8))
        def _():
            others(a, lambda i, to: d_pl(i, to, a).start())

    work(0, -3, True)
    work(0, 3, True)
    onward(1, 2, 0)
    onward(1, 2, 1)
    work(1, -2, True)
    work(1, 2, True)
    last_hop(1, 0)
    last_hop(1, 1)
    @pl.when(a != 0)
    def _():
        d_pl(0, 0, 0).wait_recv()

    @pl.when((a != 1) & (b >= 8))
    def _():
        d_pl(0, 1, 1).wait_recv()

    @pl.when(b < 8)
    def _():
        others(b, lambda i, to: d_ag(i, to, b, 1).start())

    @pl.when(b >= 8)
    def _():
        others(b, lambda i, to: d_ag(i, to, b, 2).start())
        dring[k, b, 1] = dpc[1]

    dring[k, b, 0] = dpc[0]
    arrive(slot(0, 4), 0)
    arrive(slot(0, 4), 1)
    work(0, 4, True)
    work(1, -3, True)
    work(1, 3, True)
    arrive(slot(1, 4), 0)
    arrive(slot(1, 4), 1)
    work(1, 4, True)

    @pl.when(a >= 2)
    def _():
        @pl.loop(0, 2)
        def _(i):
            dprod[i] = dot(xb[i], lhs[...], 0, 0)

    others(b, lambda i, to: p_rs(i, to).start())
    pland[b] = own_rows(dprod)
    for n, who in held:
        multiply(n, who)

    others(b, lambda i, frm: sq_b(i, b, frm).wait_recv())
    sqv[2] = total_of(sqb)
    sq_swap = copy(sqv.at[2], sqo, s_core.at[1], r_core.at[1], partner)
    sq_swap.start()

    @pl.loop(0, 8)
    def _(p):
        @pl.when(p != b)
        def _():
            d_ag(0, b, p, 1).wait_recv()

        @pl.when(p + 8 != b)
        def _():
            d_ag(0, b, p + 8, 2).wait_recv()

    d_swap = copy(dring.at[k], dring.at[k], s_core.at[2], r_core.at[2], partner)
    d_swap.start()
    sq_swap.wait_recv()
    both = sqv[2] + sqo[...]
    squares = jnp.sum(jnp.sum(both, axis=0, keepdims=True), axis=1, keepdims=True)
    fro_ref[0] = jnp.sqrt(squares)[0, 0]
    scale = weight_ref[0] / squares
    row0 = a * 256 + k * 128
    col0 = b * 256

    def iota(shape, dim, start=0):
        return lax.broadcasted_iota(jnp.int32, shape, dim) + start

    def scaled(v, r0, c0):
        eye = (iota(v.shape, 0, r0) == iota(v.shape, 1, c0)).astype(F32)
        return v * scale + eye

    copy(dring.at[1 - k], dring.at[1 - k], s_core.at[2], r_core.at[2], partner).wait_recv()
    for kk in range(2):
        for i in range(2):
            r = i * 256 + kk * 128
            for j in range(i + 1):
                v = dring[kk, 8 * i : 8 * i + 8, j].reshape(128, 256)
                s[r : r + 128, 256 * j : 256 * j + 256] = scaled(v, r, 256 * j)

    to_mirror = copy(red, gpiece, s_mir.at[0], r_mir.at[0], mirror)
    turn = copy(turned, half_in, s_mir.at[1], r_mir.at[1], mirror)
    trade = copy(
        turned.at[:, pl.ds(pl.multiple_of((1 - k) * 128, 128), 128)],
        half_in.at[:, 0:128],
        s_core.at[3], r_core.at[3], partner,
    )

    def hook_rows():
        others(b, lambda i, frm: p_rs(i, frm, frm).wait_recv())
        red[...] = total_of(pland)

        @pl.when(a != b)
        def _():
            to_mirror.start()

        others(b, lambda i, to: p_ag(i, to).start())
        pring[k, b] = red[...]

        @pl.when(a == b)
        def _():
            gpiece[...] = red[...]

    to_twin = copy(part, hland, s_h.at[0], r_h.at[0], (x, y, k, z, 1 - h))

    def sum_over_z(side, who):
        pile[side, z] = prod[who]

        @pl.loop(1, 8)
        def _(i):
            frm = lax.rem(z + i, 8)
            copy(
                prod.at[who], pile.at[side, frm], s_a2a.at[0], r_a2a.at[side * 8 + frm],
                (x, y, k, frm, h),
            ).wait_recv()

        v = pile[side, 0]
        for i in range(1, 8):
            v = v + pile[side, i]
        return v

    def hook_half():
        @pl.when(helps)
        def _():
            part[...] = sum_over_z(1 - h, twin)
            to_twin.start()

        @pl.when(mine)
        def _():
            turned[...] = sum_over_z(h, b)

    def hook_tile():
        @pl.when(mine)
        def _():
            to_twin.wait_recv()
            turned[...] = turned[...] + hland[...]
            trade.start()

            @pl.when(a != b)
            def _():
                turn.start()

    def hook_mirror():
        @pl.when(a != b)
        def _():
            to_mirror.wait_recv()

        others(a, lambda i, to: g_pl(i, to).start())
        gring[k, a] = gpiece[...]

    p_swap = copy(pring.at[k], pring.at[k], s_core.at[4], r_core.at[4], partner)
    g_swap = copy(gring.at[k], gring.at[k], s_core.at[5], r_core.at[5], partner)

    def hook_last():
        others(b, lambda i, frm: p_ag(i, b, frm).wait_recv())
        p_swap.start()

    def hook_rest():
        others(a, lambda i, frm: g_pl(i, a, frm).wait_recv())
        g_swap.start()

    def idle():
        pass

    factor_pair(
        s, inv_ref, cross, w,
        [idle, idle, hook_rows, hook_half, hook_mirror, hook_tile, hook_last, hook_rest],
    )

    copy(pring.at[1 - k], pring.at[1 - k], s_core.at[4], r_core.at[4], partner).wait_recv()
    copy(gring.at[1 - k], gring.at[1 - k], s_core.at[5], r_core.at[5], partner).wait_recv()
    for kk in range(2):
        for i in range(2):
            r = i * 256 + kk * 128
            v = pring[kk, 8 * i : 8 * i + 8, :, pl.ds(pl.multiple_of(k * 128, 128), 128)].reshape(128, 128)
            g[r : r + 128, 0:128] = scaled(v, r, row0)
            v = gring[kk, 8 * i : 8 * i + 8].reshape(128, 256)
            g[r : r + 128, 128:384] = scaled(v, r, col0)

    lane = iota((256, 384), 1)
    ids = lane + jnp.where(lane < 128, row0, col0 - 128)
    first = iota((256, 384), 0)
    one = jnp.where(ids >= first, dot(inv_ref[0], g[0:256, :]), 0.0)
    low[0:256, :] = one
    two = dot(inv_ref[1], g[256:512, :] - dot(cross[...], one))
    low[256:512, :] = jnp.where(ids >= first + 256, two, 0.0)
    pan_ref[...] = low[:, 0:128].T
    less = dot(low[:, 0:128], low[:, 128:384], 0, 0)

    @pl.when(mine)
    def _():
        own = pl.ds(pl.multiple_of(k * 128, 128), 128)
        out_ref[:, own] = turned[:, own].T
        trade.wait_recv()
        out_ref[:, pl.ds(pl.multiple_of((1 - k) * 128, 128), 128)] = half_in[:, 0:128].T

    @pl.when(chosen(b, a) & (a != b))
    def _():
        turn.wait_recv()
        out_ref[...] = half_in[...]

    out_ref[...] = scaled(out_ref[...], row0, col0) - less

    for c in sent:
        c.wait_send()
    to_core.wait_send()
    sq_swap.wait_send()
    d_swap.wait_send()
    p_swap.wait_send()
    g_swap.wait_send()

    @pl.when(mine)
    def _():
        trade.wait_send()

    @pl.when(mine & (a != b))
    def _():
        turn.wait_send()

    @pl.when(helps)
    def _():
        to_twin.wait_send()

    @pl.when(a != b)
    def _():
        to_mirror.wait_send()

    @pl.when(a < 2)
    def _():
        others(b, lambda i, to: d_rs(i, to).wait_send())

    @pl.when((a == 0) | ((a == 1) & (b >= 8)))
    def _():
        others(a, lambda i, to: d_pl(i, to, a).wait_send())

    @pl.when(b < 8)
    def _():
        others(b, lambda i, to: d_ag(i, to, b, 1).wait_send())

    @pl.when(b >= 8)
    def _():
        others(b, lambda i, to: d_ag(i, to, b, 2).wait_send())

    others(a, lambda i, to: sq_a(i, to).wait_send())
    others(b, lambda i, to: sq_b(i, to).wait_send())
    others(b, lambda i, to: p_rs(i, to).wait_send())
    others(b, lambda i, to: p_ag(i, to).wait_send())
    others(a, lambda i, to: g_pl(i, to).wait_send())
    for n, who in enumerate(tiles):

        @pl.when(chosen(a, who) & (lax.div(who, 2) != z))
        def _():
            tile(n, who).wait_send()


def on_device(x_slab, weight_c):
    vmem, smem = pl.BlockSpec(memory_space=pltpu.VMEM), pl.BlockSpec(memory_space=pltpu.SMEM)
    dma = pltpu.SemaphoreType.DMA
    shapes = [(128, 256), (128, 512), (2, 256, 256), (1,)]
    scratch = [
        (16, 512, 128), (512, 128), (512, 256), (16, 128, 256), (2, 128, 256), (16, 16, 256),
        (2, 16, 256), (2, 16, 2, 16, 256), (16, 16, 256), (16, 256), (2, 16, 16, 256), (16, 256),
        (2, 16, 16, 256), (2, 8, 128, 256), (128, 256), (128, 256), (128, 256), (128, 256), (3, 8, 128), (16, 8, 128),
        (16, 8, 128), (8, 128), (512, 512), (128, 128), (256, 256), (512, 384), (512, 384),
    ]
    sems = [40, 32, 6, 6, 16, 16, 16, 2, 16, 16, 16, 16, 16, 16, 16, 16, 16, 16, 1, 1, 2, 2, 16, 16, 16, 16]
    return pl.pallas_call(
        step_kernel,
        out_shape=[jax.ShapeDtypeStruct(s, F32) for s in shapes],
        in_specs=[smem, vmem],
        out_specs=[vmem] * 3 + [smem],
        scratch_shapes=[pltpu.VMEM(s, F32) for s in scratch] + [dma((n,)) for n in sems],
        compiler_params=pltpu.CompilerParams(
            collective_id=0, has_side_effects=True, vmem_limit_bytes=48 * 1024 * 1024
        ),
        name="step",
    )(weight_c, x_slab)


def solution(mesh):
    split = Mesh(mesh.devices.reshape(2, 8, 2, 8, 2), AXES)
    return jax.shard_map(
        on_device, mesh=split, in_specs=(P(COL, ROW), P()),
        out_specs=(P(ROW, COL), P(ROW, None), P(), P()), check_vma=False,
    )
```
